256 devices in a mesh: groups: 4 (over y, x), row: 64 (over z, core).
Axes of the slice: x: 2, y: 2, z: 32, core: 2. Of those that a mesh axis runs over, the one named last changes fastest.
The devices are a block of a 4x8x32 slice.
Arguments:
- elevation: float32 [4096, 8192], P(('groups', 'row')), parts along dimension 0, may hold values from -2048 to 4096
- bin_index: int32 [4096, 8192], P(('groups', 'row')), parts along dimension 0, may hold values from 0 to 1023, as said below
- ranks: int32 [8], P('groups'), parts along dimension 0, may hold values from 83886 to 8304713, as said below
Outputs:
- shaded: float32 [4096, 8192], P(('groups', 'row')), parts along dimension 0
The draws below stay inside these ranges and needn't reach their ends.
There are 4 independent parts, one for each index of `groups`. The reference program is written for one: setup_inputs(seed, part) draws one part's arguments, and reference() takes and returns one part's arrays. A program takes and returns all parts, laid end to end along the dimension named above; each array names one. Nothing has to cross between parts.
Inputs may be any that keep to these rules, and one draw needn't show every extreme that they name: The bins have fixed edges: a cell with 0 < bin_index < 1023 has an elevation at or above 2 bin_index and below 2 bin_index + 2; bin 0 holds every elevation below 2 and bin 1024 - 1 every elevation at or above 2046. `ranks`: the first entry lies below 419430 and the second at or above 7969170.
All inputs are finite; a program needn't handle non-finite values.
Results may differ from the reference program's by a relative error of at most 0.0049.
Values sent between devices are 32-bit elements; how exact they have to be, the bound alone decides.
No kernel may reach another device: no remote copies, remote signals or barrier semaphores. Data moves between devices by JAX's collectives and lax.ppermute only.
A program may use at most 64 MiB of HBM per device.

```python
import jax
import jax.numpy as jnp
from jax import lax

COLS = 8192
BINS = 1024
NROWS = 1024
TOTAL = 8388608


def relief_bins(key):
    subkeys = jax.random.split(key, 6)
    amplitude = jax.random.randint(subkeys[0], (), BINS // 4, BINS * 3 // 4, jnp.int32)
    offset = jax.random.randint(subkeys[1], (), 0, BINS - amplitude - 64, jnp.int32)
    curvature = jax.random.randint(subkeys[2], (), -(BINS // 8), BINS // 8 + 1, jnp.int32)
    column_tilt = jax.random.randint(subkeys[3], (), 0, 48, jnp.int32)
    reversed_trend = jax.random.randint(subkeys[4], (), 0, 2, jnp.int32)
    roughness = jax.random.randint(subkeys[5], (NROWS, COLS), -6, 7, jnp.int32)
    row_fraction = jnp.arange(NROWS, dtype=jnp.int32) * 1024 // NROWS
    row_trend = jnp.where(reversed_trend == 1, 1023 - row_fraction, row_fraction)
    row_term = amplitude * row_trend // 1024 + curvature * row_trend * (1023 - row_trend) // 262144
    column_fraction = jnp.arange(COLS, dtype=jnp.int32) * 1024 // COLS
    column_term = column_tilt * column_fraction // 1024
    field = offset + 32 + row_term[:, None] + column_term[None, :] + roughness
    lowest = jnp.min(field)
    spread = jnp.maximum(jnp.max(field) - lowest, 1)
    scaled = (field - lowest) * (BINS + 76) // spread - 38
    return jnp.clip(scaled, 0, BINS - 1).astype(jnp.int32)


def draw_bin_index(key, part):
    return relief_bins(jax.random.fold_in(key, 7))


def draw_elevation(key, part):
    bin_field = relief_bins(jax.random.fold_in(key, 7))
    offset_key = jax.random.fold_in(key, 8)
    excess_keys = jax.random.split(jax.random.fold_in(key, 9), 3)
    top_extent = jax.random.uniform(excess_keys[0], (), jnp.float32, BINS * 0.5, BINS * 2.0)
    bottom_extent = jax.random.uniform(excess_keys[1], (), jnp.float32, BINS * 0.5, BINS * 2.0)
    unit = jax.random.uniform(excess_keys[2], (NROWS, COLS), jnp.float32, 0.0, 0.999)
    fraction = 0.5 + 0.15 * jax.random.truncated_normal(offset_key, -3.2, 3.2, (NROWS, COLS), jnp.float32)
    profile = unit * unit
    base = 2.0 * (bin_field.astype(jnp.float32) + fraction)
    raised = jnp.where(bin_field == BINS - 1, top_extent * profile, 0.0)
    lowered = jnp.where(bin_field == 0, bottom_extent * profile, 0.0)
    return base + raised - lowered


def draw_ranks(key, part):
    first, second = jax.random.split(key, 2)
    lower = jax.random.randint(first, (1,), TOTAL // 100, TOTAL // 20, jnp.int32)
    upper = jax.random.randint(second, (1,), TOTAL // 100 * 95, TOTAL // 100 * 99, jnp.int32)
    return jnp.concatenate([lower, upper])


def setup_inputs(seed: int = 0, part: int = 0) -> dict:
    splits = jax.random.split(jax.random.key(seed), 4)
    part_splits = jax.random.split(jax.random.fold_in(splits[3], part), 4)
    elevation = draw_elevation(jax.random.fold_in(jax.random.fold_in(splits[3], part), 71), part)
    bin_index = draw_bin_index(jax.random.fold_in(jax.random.fold_in(splits[3], part), 71), part)
    ranks = draw_ranks(jax.random.fold_in(jax.random.fold_in(splits[3], part), 71), part)
    return dict(elevation=elevation, bin_index=bin_index, ranks=ranks)


binomial = (1.0 / 64, 6.0 / 64, 15.0 / 64, 20.0 / 64, 15.0 / 64, 6.0 / 64, 1.0 / 64)
zfactor = 200.0
cos_zenith = 0.70710678
sin_zenith = 0.70710678
light_x = -0.70710678
light_y = 0.70710678

def filter_cols(padded):
    width = padded.shape[1] - 6
    total = binomial[0] * padded[:, 0:width]
    for offset in range(1, 7):
        total = total + binomial[offset] * padded[:, offset:offset + width]
    return total

def filter_rows(padded):
    height = padded.shape[0] - 6
    total = binomial[0] * padded[0:height, :]
    for offset in range(1, 7):
        total = total + binomial[offset] * padded[offset:offset + height, :]
    return total

def shade(smooth, span):
    height = smooth.shape[0] - 2
    width = smooth.shape[1] - 2

    def window(drow, dcol):
        return smooth[drow:drow + height, dcol:dcol + width]
    east = window(0, 2) + 2.0 * window(1, 2) + window(2, 2)
    west = window(0, 0) + 2.0 * window(1, 0) + window(2, 0)
    south = window(2, 0) + 2.0 * window(2, 1) + window(2, 2)
    north = window(0, 0) + 2.0 * window(0, 1) + window(0, 2)
    scale = zfactor / (8.0 * span)
    grad_x = (east - west) * scale
    grad_y = (south - north) * scale
    light = (cos_zenith - sin_zenith * (light_x * grad_x + light_y * grad_y)) * lax.rsqrt(1.0 + grad_x * grad_x + grad_y * grad_y)
    return jnp.maximum(light, 0.0)

def reference(elevation, bin_index, ranks):
    counts = jnp.zeros((BINS,), jnp.float32).at[bin_index.reshape(-1)].add(1.0)
    span = jnp.max(elevation) - jnp.min(elevation)
    cumulative = jnp.cumsum(counts.astype(jnp.int32), dtype=jnp.int32)
    table = jnp.clip((cumulative - ranks[0]).astype(jnp.float32) / (ranks[1] - ranks[0]).astype(jnp.float32), 0.0, 1.0).astype(jnp.bfloat16)
    stretch = table.astype(jnp.float32)[bin_index]
    padded = jnp.pad(elevation, 4)
    smooth = filter_rows(filter_cols(padded))
    light = shade(smooth, span)
    return stretch * (0.5 + light)
```

```python
import functools

import jax
import jax.numpy as jnp
from jax import lax
from jax.experimental import pallas as pl
from jax.experimental.pallas import tpu as pltpu
from jax.sharding import PartitionSpec as P

BINS = 1024
HALF = BINS // 2
LANES = 128
LOW = 32
WIRE = HALF + LANES

zfactor = 200.0
cos_zenith = 0.70710678
sin_zenith = 0.70710678
light_x = -0.70710678
light_y = 0.70710678
HIGHEST = lax.Precision.HIGHEST


def bin_of(height):
    return jnp.clip(jnp.floor(height * 0.5), 0.0, BINS - 1.0)


def iota(shape, dim):
    return lax.broadcasted_iota(jnp.int32, shape, dim)


def count_kernel(heights, core_ref, keep_ref, send_ref, upper, lower):
    rows, width = heights.shape
    high_count = BINS // LOW
    bins = bin_of(heights[...])
    up = jnp.floor(bins * (1.0 / LOW))
    upper[...] = up
    lower[...] = bins - up * LOW
    row_ids = iota((LOW, width), 0).astype(jnp.float32)
    one = jnp.float32(1.0)
    zero = jnp.float32(0.0)

    def step(r, total):
        up_hot = jnp.where(upper[pl.ds(r, 1), :] == row_ids, one, zero).astype(jnp.bfloat16)
        low_hot = jnp.where(lower[pl.ds(r, 1), :] == row_ids, one, zero).astype(jnp.bfloat16)
        return total + lax.dot_general(
            up_hot, low_hot, (((1,), (1,)), ((), ())), preferred_element_type=jnp.float32
        )

    grid = lax.fori_loop(0, rows, step, jnp.zeros((high_count, LOW), jnp.float32))
    spread = (iota((LOW, LANES), 1) % LOW == iota((LOW, LANES), 0)).astype(jnp.float32)
    tiled = jnp.dot(grid, spread, precision=HIGHEST, preferred_element_type=jnp.float32)
    quarter = iota((high_count, LANES), 1) // LOW == iota((high_count, LANES), 0) % 4
    fold = (iota((8, high_count), 1) // 4 == iota((8, high_count), 0)).astype(jnp.float32)
    flat = jnp.dot(
        fold, jnp.where(quarter, tiled, 0.0), precision=HIGHEST, preferred_element_type=jnp.float32
    )
    highest = jnp.max(heights[...])
    neg_lowest = -jnp.min(heights[...])
    first = core_ref[0] == 0
    for i in range(4):
        cols = slice(i * LANES, (i + 1) * LANES)
        keep_ref[:, cols] = jnp.where(first, flat[i : i + 1], flat[4 + i : 5 + i])
        send_ref[:, cols] = jnp.where(first, flat[4 + i : 5 + i], flat[i : i + 1])
    keep_ref[:, HALF:] = jnp.full((1, LANES), jnp.where(first, highest, neg_lowest))
    send_ref[:, HALF:] = jnp.full((1, LANES), jnp.where(first, neg_lowest, highest))


def count(elevation, core):
    shape = jax.ShapeDtypeStruct((1, WIRE), jnp.float32)
    return pl.pallas_call(
        count_kernel,
        out_shape=(shape, shape),
        in_specs=[
            pl.BlockSpec(memory_space=pltpu.VMEM),
            pl.BlockSpec(memory_space=pltpu.SMEM),
        ],
        out_specs=(pl.BlockSpec(memory_space=pltpu.VMEM),) * 2,
        scratch_shapes=[pltpu.VMEM(elevation.shape, jnp.float32)] * 2,
    )(elevation, core)


def spread_kernel(a_ref, b_ref, out_ref):
    a, b = a_ref[...], b_ref[...]
    both = jnp.where(iota(a.shape, 1) < HALF, a + b, jnp.maximum(a, b))
    out_ref[...] = jnp.broadcast_to(both, out_ref.shape)


def gather_kernel(x_ref, out_ref):
    out_ref[:, :HALF] = jnp.sum(x_ref[:, :HALF], axis=0, keepdims=True)
    out_ref[:, HALF:] = jnp.max(x_ref[:, HALF:], axis=0, keepdims=True)


def shade_kernel(mine, theirs, core_ref, ranks, heights, gx_ref, gy_ref, out_ref):
    first = core_ref[0] == 0
    a, b = mine[...], theirs[...]
    lower = jnp.where(first, a, b)
    upper = jnp.where(first, b, a)
    span = lower[:, HALF : HALF + 1] + upper[:, HALF : HALF + 1]
    parts = [lower[:, i * LANES : (i + 1) * LANES] for i in range(4)]
    parts += [upper[:, i * LANES : (i + 1) * LANES] for i in range(4)]
    counts = jnp.concatenate(parts, axis=0)
    upto = (iota((LANES, LANES), 0) <= iota((LANES, LANES), 1)).astype(jnp.float32)
    inside = jnp.dot(counts, upto, precision=HIGHEST, preferred_element_type=jnp.float32)
    ones = jnp.ones((LANES, LANES), jnp.float32)
    totals = jnp.dot(counts, ones, precision=HIGHEST, preferred_element_type=jnp.float32)
    before = (iota((8, 8), 1) < iota((8, 8), 0)).astype(jnp.float32)
    ahead = jnp.dot(before, totals, precision=HIGHEST, preferred_element_type=jnp.float32)
    cumulative = (inside + ahead).astype(jnp.int32)
    table = jnp.clip(
        (cumulative - ranks[0]).astype(jnp.float32)
        / jnp.full(cumulative.shape, ranks[1] - ranks[0]).astype(jnp.float32),
        0.0,
        1.0,
    )
    table = table.astype(jnp.bfloat16).astype(jnp.float32)
    rows, width = heights.shape
    scale = zfactor / (8.0 * span)
    tables = [jnp.broadcast_to(table[r : r + 1], (rows, LANES)) for r in range(8)]
    for c in range(width // LANES):
        cols = slice(c * LANES, (c + 1) * LANES)
        bins = bin_of(heights[:, cols]).astype(jnp.int32)
        low = bins & (LANES - 1)
        high = bins >> 7
        found = [
            jnp.take_along_axis(t, low, axis=1, mode="promise_in_bounds") for t in tables
        ]
        for bit in range(3):
            odd = (high & (1 << bit)) != 0
            found = [jnp.where(odd, found[2 * i + 1], found[2 * i]) for i in range(len(found) // 2)]
        gx = gx_ref[:, cols] * scale
        gy = gy_ref[:, cols] * scale
        light = (cos_zenith - sin_zenith * (light_x * gx + light_y * gy)) * lax.rsqrt(
            1.0 + gx * gx + gy * gy
        )
        out_ref[:, cols] = found[0] * (0.5 + jnp.maximum(light, 0.0))


def shade(mine, theirs, core, ranks, elevation, gx, gy):
    vmem = pl.BlockSpec(memory_space=pltpu.VMEM)
    smem = pl.BlockSpec(memory_space=pltpu.SMEM)
    return pl.pallas_call(
        shade_kernel,
        out_shape=jax.ShapeDtypeStruct(elevation.shape, jnp.float32),
        in_specs=[vmem, vmem, smem, smem, vmem, vmem, vmem],
        out_specs=vmem,
    )(mine, theirs, core, ranks, elevation, gx, gy)


def pairs_added(x, times, dim):
    for _ in range(times):
        n = x.shape[dim] - 1
        x = lax.slice_in_dim(x, 0, n, axis=dim) + lax.slice_in_dim(x, 1, n + 1, axis=dim)
    return x


def gradients(extended):
    common = pairs_added(extended, 7, 0)
    common = pairs_added(jnp.pad(common, ((0, 0), (4, 4))), 7, 1) * (1.0 / 4096)
    east = common[:, 1:] - common[:, :-1]
    south = common[:, 1:] + common[:, :-1]
    return east[1:] + east[:-1], south[1:] - south[:-1]


def body(elevation, ranks):
    size = lax.axis_size("row")
    core = (lax.axis_index("row") % 2).astype(jnp.int32).reshape(1)
    partner = [(i, i ^ 1) for i in range(size)]
    same_core = [list(range(c, size, 2)) for c in range(2)]
    keep, send = count(elevation, core)
    received = lax.ppermute(send, "row", partner)
    spread = pl.pallas_call(
        spread_kernel, out_shape=jax.ShapeDtypeStruct((size // 2, WIRE), jnp.float32)
    )(keep, received)
    everyone = lax.all_to_all(spread, "row", 0, 0, axis_index_groups=same_core, tiled=True)

    head = elevation[:4]
    tail = elevation[-4:]
    above = lax.ppermute(tail, "row", [(i, i + 1) for i in range(size - 1)])
    below = lax.ppermute(head, "row", [(i + 1, i) for i in range(size - 1)])
    gx, gy = gradients(jnp.concatenate([above, elevation, below], axis=0))

    mine = pl.pallas_call(
        gather_kernel, out_shape=jax.ShapeDtypeStruct((1, WIRE), jnp.float32)
    )(everyone)
    theirs = lax.ppermute(mine, "row", partner)
    return shade(mine, theirs, core, ranks, elevation, gx, gy)


def solution(mesh):
    whole = P(("groups", "row"), None)
    mapped = jax.shard_map(
        body, mesh=mesh, in_specs=(whole, P("groups")), out_specs=whole, check_vma=False
    )

    def run(elevation, bin_index, ranks):
        return mapped(elevation, ranks)

    return run
```

```python
import jax
import jax.numpy as jnp
from jax import lax
from jax.experimental import pallas as pl
from jax.experimental.pallas import tpu as pltpu
from jax.sharding import PartitionSpec as P

BINS = 1024
HALF = BINS // 2
LANES = 128
LOW = 32
WIRE = HALF + LANES

zfactor = 200.0
cos_zenith = 0.70710678
sin_zenith = 0.70710678
light_x = -0.70710678
light_y = 0.70710678
HIGHEST = lax.Precision.HIGHEST


def bin_of(height):
    return jnp.clip(jnp.floor(height * 0.5), 0.0, BINS - 1.0)


def iota(shape, dim):
    return lax.broadcasted_iota(jnp.int32, shape, dim)


def in_vmem(x):
    return pltpu.with_memory_space_constraint(x, pltpu.VMEM)


def count_kernel(heights, core_ref, keep_ref, send_ref, upper, lower):
    rows, width = heights.shape
    high_count = BINS // LOW
    bins = bin_of(heights[...])
    up = jnp.floor(bins * (1.0 / LOW))
    upper[...] = up
    lower[...] = bins - up * LOW
    row_ids = iota((LOW, width), 0).astype(jnp.float32)
    one = jnp.float32(1.0)
    zero = jnp.float32(0.0)
    grid = jnp.zeros((high_count, LOW), jnp.float32)
    for r in range(rows):
        up_hot = jnp.where(upper[r : r + 1, :] == row_ids, one, zero).astype(jnp.bfloat16)
        low_hot = jnp.where(lower[r : r + 1, :] == row_ids, one, zero).astype(jnp.bfloat16)
        grid = grid + lax.dot_general(
            up_hot, low_hot, (((1,), (1,)), ((), ())), preferred_element_type=jnp.float32
        )
    spread = (iota((LOW, LANES), 1) % LOW == iota((LOW, LANES), 0)).astype(jnp.float32)
    tiled = jnp.dot(grid, spread, precision=HIGHEST, preferred_element_type=jnp.float32)
    quarter = iota((high_count, LANES), 1) // LOW == iota((high_count, LANES), 0) % 4
    fold = (iota((8, high_count), 1) // 4 == iota((8, high_count), 0)).astype(jnp.float32)
    flat = jnp.dot(
        fold, jnp.where(quarter, tiled, 0.0), precision=HIGHEST, preferred_element_type=jnp.float32
    )
    highest = jnp.max(heights[...])
    neg_lowest = -jnp.min(heights[...])
    first = core_ref[0] == 0
    for i in range(4):
        cols = slice(i * LANES, (i + 1) * LANES)
        keep_ref[:, cols] = jnp.where(first, flat[i : i + 1], flat[4 + i : 5 + i])
        send_ref[:, cols] = jnp.where(first, flat[4 + i : 5 + i], flat[i : i + 1])
    keep_ref[:, HALF:] = jnp.full((1, LANES), jnp.where(first, highest, neg_lowest))
    send_ref[:, HALF:] = jnp.full((1, LANES), jnp.where(first, neg_lowest, highest))


VMEM_SPEC = pl.BlockSpec(memory_space=pltpu.VMEM)
SMEM_SPEC = pl.BlockSpec(memory_space=pltpu.SMEM)


def count(elevation, core):
    shape = pltpu.VMEM((1, WIRE), jnp.float32)
    return pl.pallas_call(
        count_kernel,
        out_shape=(shape, shape),
        in_specs=[VMEM_SPEC, SMEM_SPEC],
        out_specs=(VMEM_SPEC,) * 2,
        scratch_shapes=[pltpu.VMEM(elevation.shape, jnp.float32)] * 2,
        name="count",
    )(elevation, core)


def join_kernel(a_ref, b_ref, out_ref):
    a, b = a_ref[...], b_ref[...]
    both = jnp.where(iota(a.shape, 1) < HALF, a + b, jnp.maximum(a, b))
    out_ref[...] = jnp.broadcast_to(both[None], out_ref.shape)


def join(a, b, copies):
    return pl.pallas_call(
        join_kernel,
        out_shape=pltpu.VMEM((copies, *a.shape), jnp.float32),
        in_specs=[VMEM_SPEC] * 2,
        out_specs=VMEM_SPEC,
        name="join",
    )(a, b)


def gather_kernel(x_ref, out_ref):
    x = x_ref[...]
    out_ref[:, :HALF] = jnp.sum(x[:, :, :HALF], axis=0)
    out_ref[:, HALF:] = jnp.max(x[:, :, HALF:], axis=0)


def gather(everyone):
    return pl.pallas_call(
        gather_kernel,
        out_shape=pltpu.VMEM((1, WIRE), jnp.float32),
        in_specs=[VMEM_SPEC],
        out_specs=VMEM_SPEC,
        name="gather",
    )(everyone)


def gradient_kernel(above, middle, below, gx_ref, gy_ref, wide):
    rows, width = middle.shape
    halo = above.shape[0]
    edge = jnp.zeros((rows + 2 * halo, LANES), jnp.float32)
    wide[:, :LANES] = edge
    wide[:, LANES + width :] = edge
    wide[:halo, LANES : LANES + width] = above[...]
    wide[halo : halo + rows, LANES : LANES + width] = middle[...]
    wide[halo + rows :, LANES : LANES + width] = below[...]
    chunk = 4 * LANES
    for c in range(0, width, chunk):
        x = wide[:, c : c + chunk + 2 * LANES]
        tall, across = x.shape
        for _ in range(7):
            x = x + pltpu.roll(x, tall - 1, 0)
        for _ in range(4):
            x = x + pltpu.roll(x, 1, 1)
        for _ in range(3):
            x = x + pltpu.roll(x, across - 1, 1)
        x = x * (1.0 / 4096)
        ahead = pltpu.roll(x, across - 1, 1)
        east = ahead - x
        both = ahead + x
        gx = east + pltpu.roll(east, tall - 1, 0)
        gy = pltpu.roll(both, tall - 1, 0) - both
        gx_ref[:, c : c + chunk] = gx[:rows, LANES : LANES + chunk]
        gy_ref[:, c : c + chunk] = gy[:rows, LANES : LANES + chunk]


def gradients(above, middle, below):
    rows, width = middle.shape
    shape = pltpu.VMEM(middle.shape, jnp.float32)
    return pl.pallas_call(
        gradient_kernel,
        out_shape=(shape, shape),
        in_specs=[VMEM_SPEC] * 3,
        out_specs=(VMEM_SPEC,) * 2,
        scratch_shapes=[
            pltpu.VMEM((rows + 2 * above.shape[0], width + 2 * LANES), jnp.float32)
        ],
        name="gradients",
    )(above, middle, below)


def shade_kernel(mine, theirs, core_ref, ranks, heights, gx_ref, gy_ref, out_ref, held, scale_ref):
    step = pl.program_id(0)

    @pl.when(step == 0)
    def _():
        first = core_ref[0] == 0
        a, b = mine[...], theirs[...]
        lower = jnp.where(first, a, b)
        upper = jnp.where(first, b, a)
        span = lower[:, HALF:] + upper[:, HALF:]
        scale_ref[...] = zfactor / (8.0 * span)
        parts = [lower[:, i * LANES : (i + 1) * LANES] for i in range(4)]
        parts += [upper[:, i * LANES : (i + 1) * LANES] for i in range(4)]
        counts = jnp.concatenate(parts, axis=0)
        upto = (iota((LANES, LANES), 0) <= iota((LANES, LANES), 1)).astype(jnp.float32)
        inside = jnp.dot(counts, upto, precision=HIGHEST, preferred_element_type=jnp.float32)
        totals = jnp.broadcast_to(jnp.sum(counts, axis=1, keepdims=True), counts.shape)
        rows = iota(counts.shape, 0)
        ahead = jnp.zeros(counts.shape, jnp.float32)
        for r in range(7):
            ahead = ahead + jnp.where(rows > r, totals[r : r + 1], 0.0)
        cumulative = (inside + ahead).astype(jnp.int32)
        table = jnp.clip(
            (cumulative - ranks[0]).astype(jnp.float32)
            / jnp.full(cumulative.shape, ranks[1] - ranks[0]).astype(jnp.float32),
            0.0,
            1.0,
        )
        held[...] = table.astype(jnp.bfloat16).astype(jnp.float32)

    rows, width = out_ref.shape
    tables = [jnp.broadcast_to(held[r : r + 1], (rows, LANES)) for r in range(8)]
    scale = scale_ref[...]
    for c in range(width // LANES):
        cols = pl.ds(pl.multiple_of(step * width + c * LANES, LANES), LANES)
        bins = bin_of(heights[:, cols]).astype(jnp.int32)
        low = bins & (LANES - 1)
        high = bins >> 7
        found = [
            jnp.take_along_axis(t, low, axis=1, mode="promise_in_bounds") for t in tables
        ]
        for bit in range(3):
            odd = (high & (1 << bit)) != 0
            found = [jnp.where(odd, found[2 * i + 1], found[2 * i]) for i in range(len(found) // 2)]
        gx = gx_ref[:, cols] * scale
        gy = gy_ref[:, cols] * scale
        light = (cos_zenith - sin_zenith * (light_x * gx + light_y * gy)) * lax.rsqrt(
            1.0 + gx * gx + gy * gy
        )
        out_ref[:, c * LANES : (c + 1) * LANES] = found[0] * (0.5 + jnp.maximum(light, 0.0))


def shade(mine, theirs, core, ranks, elevation, gx, gy):
    rows, width = elevation.shape
    steps = 4
    return pl.pallas_call(
        shade_kernel,
        grid=(steps,),
        out_shape=jax.ShapeDtypeStruct(elevation.shape, jnp.float32),
        in_specs=[VMEM_SPEC, VMEM_SPEC, SMEM_SPEC, SMEM_SPEC, VMEM_SPEC, VMEM_SPEC, VMEM_SPEC],
        out_specs=pl.BlockSpec((rows, width // steps), lambda i: (0, i)),
        scratch_shapes=[pltpu.VMEM((8, LANES), jnp.float32), pltpu.VMEM((1, LANES), jnp.float32)],
        name="shade",
    )(mine, theirs, core, ranks, elevation, gx, gy)


def body(elevation, ranks):
    size = lax.axis_size("row")
    core = lax.axis_index("row") & 1
    core = core.astype(jnp.int32).reshape(1)
    partner = [(i, i ^ 1) for i in range(size)]
    chips = size // 2
    begin = chips * 5 // 8
    order = [(i + begin) % chips for i in range(chips)]
    same_core = [[2 * i + c for i in order] for c in range(2)]
    local = in_vmem(elevation)
    keep, send = count(local, core)
    received = lax.ppermute(send, "row", partner)
    spread = join(in_vmem(keep), in_vmem(received), chips)
    everyone = lax.all_to_all(spread, "row", 0, 0, axis_index_groups=same_core, tiled=True)

    above = lax.ppermute(elevation[-4:], "row", [(i, i + 1) for i in range(size - 1)])
    below = lax.ppermute(elevation[:4], "row", [(i + 1, i) for i in range(size - 1)])
    gx, gy = gradients(in_vmem(above), local, in_vmem(below))

    mine = gather(in_vmem(everyone))
    theirs = lax.ppermute(mine, "row", partner)
    return shade(
        in_vmem(mine), in_vmem(theirs), core, ranks, local, in_vmem(gx), in_vmem(gy)
    )


def solution(mesh):
    whole = P(("groups", "row"), None)
    mapped = jax.shard_map(
        body, mesh=mesh, in_specs=(whole, P("groups")), out_specs=whole, check_vma=False
    )

    def run(elevation, bin_index, ranks):
        return mapped(elevation, ranks)

    return run
```

```python
import jax
import jax.numpy as jnp
from jax import lax
from jax.experimental import pallas as pl
from jax.experimental.pallas import tpu as pltpu
from jax.sharding import PartitionSpec as P

BINS = 1024
HALF = BINS // 2
LANES = 128
LOW = 32
WIRE = HALF + LANES

zfactor = 200.0
cos_zenith = 0.70710678
sin_zenith = 0.70710678
light_x = -0.70710678
light_y = 0.70710678
HIGHEST = lax.Precision.HIGHEST


def bin_of(height):
    return jnp.clip(jnp.floor(height * 0.5), 0.0, BINS - 1.0)


def iota(shape, dim):
    return lax.broadcasted_iota(jnp.int32, shape, dim)


def in_vmem(x):
    return pltpu.with_memory_space_constraint(x, pltpu.VMEM)


def count_kernel(heights, core_ref, keep_ref, send_ref, upper, lower):
    rows, width = heights.shape
    high_count = BINS // LOW
    bins = bin_of(heights[...])
    up = jnp.floor(bins * (1.0 / LOW))
    upper[...] = up
    lower[...] = bins - up * LOW
    row_ids = iota((LOW, width), 0).astype(jnp.float32)
    one = jnp.float32(1.0)
    zero = jnp.float32(0.0)
    grid = jnp.zeros((high_count, LOW), jnp.float32)
    for r in range(rows):
        up_hot = jnp.where(upper[r : r + 1, :] == row_ids, one, zero).astype(jnp.bfloat16)
        low_hot = jnp.where(lower[r : r + 1, :] == row_ids, one, zero).astype(jnp.bfloat16)
        grid = grid + lax.dot_general(
            up_hot, low_hot, (((1,), (1,)), ((), ())), preferred_element_type=jnp.float32
        )
    spread = (iota((LOW, LANES), 1) % LOW == iota((LOW, LANES), 0)).astype(jnp.float32)
    tiled = jnp.dot(grid, spread, precision=HIGHEST, preferred_element_type=jnp.float32)
    quarter = iota((high_count, LANES), 1) // LOW == iota((high_count, LANES), 0) % 4
    fold = (iota((8, high_count), 1) // 4 == iota((8, high_count), 0)).astype(jnp.float32)
    flat = jnp.dot(
        fold, jnp.where(quarter, tiled, 0.0), precision=HIGHEST, preferred_element_type=jnp.float32
    )
    highest = jnp.max(heights[...])
    neg_lowest = -jnp.min(heights[...])
    first = core_ref[0] == 0
    for i in range(4):
        cols = slice(i * LANES, (i + 1) * LANES)
        keep_ref[:, cols] = jnp.where(first, flat[i : i + 1], flat[4 + i : 5 + i])
        send_ref[:, cols] = jnp.where(first, flat[4 + i : 5 + i], flat[i : i + 1])
    keep_ref[:, HALF:] = jnp.full((1, LANES), jnp.where(first, highest, neg_lowest))
    send_ref[:, HALF:] = jnp.full((1, LANES), jnp.where(first, neg_lowest, highest))


VMEM_SPEC = pl.BlockSpec(memory_space=pltpu.VMEM)
SMEM_SPEC = pl.BlockSpec(memory_space=pltpu.SMEM)


def count(elevation, core):
    shape = pltpu.VMEM((1, WIRE), jnp.float32)
    return pl.pallas_call(
        count_kernel,
        out_shape=(shape, shape),
        in_specs=[VMEM_SPEC, SMEM_SPEC],
        out_specs=(VMEM_SPEC,) * 2,
        scratch_shapes=[pltpu.VMEM(elevation.shape, jnp.float32)] * 2,
        name="count",
    )(elevation, core)


def join_kernel(a_ref, b_ref, out_ref):
    a, b = a_ref[...], b_ref[...]
    both = jnp.where(iota(a.shape, 1) < HALF, a + b, jnp.maximum(a, b))
    out_ref[...] = jnp.broadcast_to(both[None], out_ref.shape)


def join(a, b, copies):
    return pl.pallas_call(
        join_kernel,
        out_shape=pltpu.VMEM((copies, *a.shape), jnp.float32),
        in_specs=[VMEM_SPEC] * 2,
        out_specs=VMEM_SPEC,
        name="join",
    )(a, b)


def gather_kernel(x_ref, out_ref):
    x = x_ref[...]
    out_ref[:, :HALF] = jnp.sum(x[:, :, :HALF], axis=0)
    out_ref[:, HALF:] = jnp.max(x[:, :, HALF:], axis=0)


def gather(everyone):
    return pl.pallas_call(
        gather_kernel,
        out_shape=pltpu.VMEM((1, WIRE), jnp.float32),
        in_specs=[VMEM_SPEC],
        out_specs=VMEM_SPEC,
        name="gather",
    )(everyone)


def gradient_kernel(above, middle, below, gx_ref, gy_ref, wide):
    rows, width = middle.shape
    halo = above.shape[0]
    edge = jnp.zeros((rows + 2 * halo, LANES), jnp.float32)
    wide[:, :LANES] = edge
    wide[:, LANES + width :] = edge
    wide[:halo, LANES : LANES + width] = above[...]
    wide[halo : halo + rows, LANES : LANES + width] = middle[...]
    wide[halo + rows :, LANES : LANES + width] = below[...]
    chunk = 4 * LANES
    tall = rows + 2 * halo
    for c in range(0, width, chunk):
        x = wide[:, LANES + c : LANES + c + chunk]
        for _ in range(7):
            x = x + pltpu.roll(x, tall - 1, 0)
        wide[:, LANES + c : LANES + c + chunk] = x * (1.0 / 4096)
    for c in range(0, width, chunk):
        x = wide[:, c : c + chunk + 2 * LANES]
        across = x.shape[1]

        def moved(k):
            return pltpu.roll(x, (-k) % across, 1)[:, LANES : LANES + chunk]

        right = [moved(k) for k in range(1, 5)]
        left = [moved(-k) for k in range(1, 5)]
        d1, d2, d3, d4 = (r - l for r, l in zip(right, left))
        s1, s2, s3, s4 = (r + l for r, l in zip(right, left))
        east = d4 + 6.0 * d3 + 14.0 * (d2 + d1)
        both = s4 + 8.0 * s3 + 28.0 * s2 + 56.0 * s1 + 70.0 * x[:, LANES : LANES + chunk]
        gx = east + pltpu.roll(east, tall - 1, 0)
        gy = pltpu.roll(both, tall - 1, 0) - both
        gx_ref[:, c : c + chunk] = gx[:rows]
        gy_ref[:, c : c + chunk] = gy[:rows]


def gradients(above, middle, below):
    rows, width = middle.shape
    shape = pltpu.VMEM(middle.shape, jnp.float32)
    return pl.pallas_call(
        gradient_kernel,
        out_shape=(shape, shape),
        in_specs=[VMEM_SPEC] * 3,
        out_specs=(VMEM_SPEC,) * 2,
        scratch_shapes=[
            pltpu.VMEM((rows + 2 * above.shape[0], width + 2 * LANES), jnp.float32)
        ],
        name="gradients",
    )(above, middle, below)


def shade_kernel(mine, theirs, core_ref, ranks, heights, gx_ref, gy_ref, out_ref, done, sems):
    first = core_ref[0] == 0
    a, b = mine[...], theirs[...]
    lower = jnp.where(first, a, b)
    upper = jnp.where(first, b, a)
    span = lower[:, HALF:] + upper[:, HALF:]
    scale = zfactor / (8.0 * span)
    parts = [lower[:, i * LANES : (i + 1) * LANES] for i in range(4)]
    parts += [upper[:, i * LANES : (i + 1) * LANES] for i in range(4)]
    counts = jnp.concatenate(parts, axis=0)
    upto = (iota((LANES, LANES), 0) <= iota((LANES, LANES), 1)).astype(jnp.float32)
    inside = jnp.dot(counts, upto, precision=HIGHEST, preferred_element_type=jnp.float32)
    totals = jnp.broadcast_to(jnp.sum(counts, axis=1, keepdims=True), counts.shape)
    row_ids = iota(counts.shape, 0)
    ahead = jnp.zeros(counts.shape, jnp.float32)
    for r in range(7):
        ahead = ahead + jnp.where(row_ids > r, totals[r : r + 1], 0.0)
    cumulative = (inside + ahead).astype(jnp.int32)
    table = jnp.clip(
        (cumulative - ranks[0]).astype(jnp.float32)
        / jnp.full(cumulative.shape, ranks[1] - ranks[0]).astype(jnp.float32),
        0.0,
        1.0,
    )
    table = table.astype(jnp.bfloat16).astype(jnp.float32)

    rows, width = heights.shape
    tables = [jnp.broadcast_to(table[r : r + 1], (rows, LANES)) for r in range(8)]
    pieces = sems.shape[0]
    piece = width // pieces
    copies = []
    for c in range(width // LANES):
        cols = slice(c * LANES, (c + 1) * LANES)
        bins = bin_of(heights[:, cols]).astype(jnp.int32)
        low = bins & (LANES - 1)
        high = bins >> 7
        found = [
            jnp.take_along_axis(t, low, axis=1, mode="promise_in_bounds") for t in tables
        ]
        for bit in range(3):
            odd = (high & (1 << bit)) != 0
            found = [jnp.where(odd, found[2 * i + 1], found[2 * i]) for i in range(len(found) // 2)]
        gx = gx_ref[:, cols] * scale
        gy = gy_ref[:, cols] * scale
        light = (cos_zenith - sin_zenith * (light_x * gx + light_y * gy)) * lax.rsqrt(
            1.0 + gx * gx + gy * gy
        )
        done[:, cols] = found[0] * (0.5 + jnp.maximum(light, 0.0))
        if (c + 1) * LANES % piece == 0:
            n = len(copies)
            span_cols = slice(n * piece, (n + 1) * piece)
            copies.append(
                pltpu.make_async_copy(done.at[:, span_cols], out_ref.at[:, span_cols], sems.at[n])
            )
            copies[-1].start()
    for copy in copies:
        copy.wait()


def shade(mine, theirs, core, ranks, elevation, gx, gy):
    return pl.pallas_call(
        shade_kernel,
        out_shape=jax.ShapeDtypeStruct(elevation.shape, jnp.float32),
        in_specs=[VMEM_SPEC, VMEM_SPEC, SMEM_SPEC, SMEM_SPEC, VMEM_SPEC, VMEM_SPEC, VMEM_SPEC],
        out_specs=pl.BlockSpec(memory_space=pl.ANY),
        scratch_shapes=[
            pltpu.VMEM(elevation.shape, jnp.float32),
            pltpu.SemaphoreType.DMA((8,)),
        ],
        name="shade",
    )(mine, theirs, core, ranks, elevation, gx, gy)


def body(elevation, ranks):
    size = lax.axis_size("row")
    core = lax.axis_index("row") & 1
    core = core.astype(jnp.int32).reshape(1)
    partner = [(i, i ^ 1) for i in range(size)]
    chips = size // 2
    begin = chips * 3 // 4
    order = [(i + begin) % chips for i in range(chips)]
    same_core = [[2 * i + c for i in order] for c in range(2)]
    local = in_vmem(elevation)
    keep, send = count(local, core)
    received = lax.ppermute(send, "row", partner)
    spread = join(in_vmem(keep), in_vmem(received), chips)
    everyone = lax.all_to_all(spread, "row", 0, 0, axis_index_groups=same_core, tiled=True)

    above = lax.ppermute(elevation[-4:], "row", [(i, i + 1) for i in range(size - 1)])
    below = lax.ppermute(elevation[:4], "row", [(i + 1, i) for i in range(size - 1)])
    gx, gy = gradients(in_vmem(above), local, in_vmem(below))

    mine = gather(in_vmem(everyone))
    theirs = lax.ppermute(mine, "row", partner)
    return shade(
        in_vmem(mine), in_vmem(theirs), core, ranks, local, in_vmem(gx), in_vmem(gy)
    )


def solution(mesh):
    whole = P(("groups", "row"), None)
    mapped = jax.shard_map(
        body, mesh=mesh, in_specs=(whole, P("groups")), out_specs=whole, check_vma=False
    )

    def run(elevation, bin_index, ranks):
        return mapped(elevation, ranks)

    return run
```

```python
import jax
import jax.numpy as jnp
from jax import lax
from jax.experimental import pallas as pl
from jax.experimental.pallas import tpu as pltpu
from jax.sharding import PartitionSpec as P

BINS = 1024
HALF = BINS // 2
LANES = 128
LOW = 32
WIRE = HALF + LANES

zfactor = 200.0
cos_zenith = 0.70710678
sin_zenith = 0.70710678
light_y = 0.70710678
HIGHEST = lax.Precision.HIGHEST
HOT = jnp.float8_e4m3fn
STEPS = 65535.0


def bin_of(height):
    return jnp.clip(jnp.floor(height * 0.5), 0.0, BINS - 1.0)


def iota(shape, dim):
    return lax.broadcasted_iota(jnp.int32, shape, dim)


def in_vmem(x):
    return pltpu.with_memory_space_constraint(x, pltpu.VMEM)


def count_kernel(heights, core_ref, keep_ref, send_ref, upper, lower):
    rows, width = heights.shape
    high_count = BINS // LOW
    bins = bin_of(heights[...])
    up = jnp.floor(bins * (1.0 / LOW))
    upper[...] = up
    lower[...] = bins - up * LOW
    row_ids = iota((LOW, width), 0).astype(jnp.float32).astype(jnp.bfloat16)
    one = jnp.array(1, HOT)
    zero = jnp.array(0, HOT)

    def hot(digits, r):
        again = digits[pl.ds(r, LOW // 2, stride=0), :].astype(jnp.bfloat16)
        return jnp.where(jnp.concatenate([again, again], axis=0) == row_ids, one, zero)

    grid = jnp.zeros((high_count, LOW), jnp.float32)
    for r in range(rows):
        grid = grid + lax.dot_general(
            hot(upper, r),
            hot(lower, r),
            (((1,), (1,)), ((), ())),
            preferred_element_type=jnp.float32,
        )
    spread = (iota((LOW, LANES), 1) % LOW == iota((LOW, LANES), 0)).astype(jnp.float32)
    tiled = jnp.dot(grid, spread, precision=HIGHEST, preferred_element_type=jnp.float32)
    quarter = iota((high_count, LANES), 1) // LOW == iota((high_count, LANES), 0) % 4
    fold = (iota((8, high_count), 1) // 4 == iota((8, high_count), 0)).astype(jnp.float32)
    flat = jnp.dot(
        fold, jnp.where(quarter, tiled, 0.0), precision=HIGHEST, preferred_element_type=jnp.float32
    )
    highest = jnp.max(heights[...])
    neg_lowest = -jnp.min(heights[...])
    first = core_ref[0] == 0
    for i in range(4):
        cols = slice(i * LANES, (i + 1) * LANES)
        keep_ref[:, cols] = jnp.where(first, flat[i : i + 1], flat[4 + i : 5 + i])
        send_ref[:, cols] = jnp.where(first, flat[4 + i : 5 + i], flat[i : i + 1])
    keep_ref[:, HALF:] = jnp.full((1, LANES), jnp.where(first, highest, neg_lowest))
    send_ref[:, HALF:] = jnp.full((1, LANES), jnp.where(first, neg_lowest, highest))


VMEM_SPEC = pl.BlockSpec(memory_space=pltpu.VMEM)
SMEM_SPEC = pl.BlockSpec(memory_space=pltpu.SMEM)


def count(elevation, core):
    shape = pltpu.VMEM((1, WIRE), jnp.float32)
    return pl.pallas_call(
        count_kernel,
        out_shape=(shape, shape),
        in_specs=[VMEM_SPEC, SMEM_SPEC],
        out_specs=(VMEM_SPEC,) * 2,
        scratch_shapes=[pltpu.VMEM(elevation.shape, jnp.float32)] * 2,
        name="count",
    )(elevation, core)


def join_kernel(a_ref, b_ref, out_ref):
    a, b = a_ref[...], b_ref[...]
    both = jnp.where(iota(a.shape, 1) < HALF, a + b, jnp.maximum(a, b))
    out_ref[...] = jnp.broadcast_to(both[None], out_ref.shape)


def join(a, b, copies):
    return pl.pallas_call(
        join_kernel,
        out_shape=pltpu.VMEM((copies, *a.shape), jnp.float32),
        in_specs=[VMEM_SPEC] * 2,
        out_specs=VMEM_SPEC,
        name="join",
    )(a, b)


def gather_kernel(x_ref, out_ref):
    x = x_ref[...]
    out_ref[:, :HALF] = jnp.sum(x[:, :, :HALF], axis=0)
    out_ref[:, HALF:] = jnp.max(x[:, :, HALF:], axis=0)


def gather(everyone):
    return pl.pallas_call(
        gather_kernel,
        out_shape=pltpu.VMEM((1, WIRE), jnp.float32),
        in_specs=[VMEM_SPEC],
        out_specs=VMEM_SPEC,
        name="gather",
    )(everyone)


def gradient_kernel(above, middle, below, gx_ref, gy_ref, bin_ref, wide):
    rows, width = middle.shape
    halo = above.shape[0]
    edge = jnp.zeros((rows + 2 * halo, LANES), jnp.float32)
    wide[:, :LANES] = edge
    wide[:, LANES + width :] = edge
    wide[:halo, LANES : LANES + width] = above[...]
    wide[halo : halo + rows, LANES : LANES + width] = middle[...]
    wide[halo + rows :, LANES : LANES + width] = below[...]
    chunk = 4 * LANES
    tall = rows + 2 * halo
    for c in range(0, width, chunk):
        x = wide[:, LANES + c : LANES + c + chunk]
        for _ in range(7):
            x = x + pltpu.roll(x, tall - 1, 0)
        wide[:, LANES + c : LANES + c + chunk] = x * (1.0 / 4096)
    for c in range(0, width, chunk):
        x = wide[:, c : c + chunk + 2 * LANES]
        across = x.shape[1]

        def moved(k):
            return pltpu.roll(x, (-k) % across, 1)[:, LANES : LANES + chunk]

        right = [moved(k) for k in range(1, 5)]
        left = [moved(-k) for k in range(1, 5)]
        d1, d2, d3, d4 = (r - l for r, l in zip(right, left))
        s1, s2, s3, s4 = (r + l for r, l in zip(right, left))
        east = d4 + 6.0 * d3 + 14.0 * (d2 + d1)
        both = s4 + 8.0 * s3 + 28.0 * s2 + 56.0 * s1 + 70.0 * x[:, LANES : LANES + chunk]
        gx = east + pltpu.roll(east, tall - 1, 0)
        gy = pltpu.roll(both, tall - 1, 0) - both
        bin_ref[:, c : c + chunk] = bin_of(middle[:, c : c + chunk]).astype(jnp.int32)
        gx_ref[:, c : c + chunk] = gx[:rows]
        gy_ref[:, c : c + chunk] = gy[:rows]


def gradients(above, middle, below):
    rows, width = middle.shape
    shape = pltpu.VMEM(middle.shape, jnp.float32)
    return pl.pallas_call(
        gradient_kernel,
        out_shape=(shape, shape, pltpu.VMEM(middle.shape, jnp.int32)),
        in_specs=[VMEM_SPEC] * 3,
        out_specs=(VMEM_SPEC,) * 3,
        scratch_shapes=[
            pltpu.VMEM((rows + 2 * above.shape[0], width + 2 * LANES), jnp.float32)
        ],
        name="gradients",
    )(above, middle, below)


def prefix_sums(counts):
    whole = counts.astype(jnp.int32)
    parts = [(whole >> shift) & 255 for shift in (0, 8, 16)]
    parts = jnp.concatenate(parts, axis=0).astype(jnp.float32).astype(jnp.bfloat16)
    upto = jnp.where(iota((LANES, LANES), 0) <= iota((LANES, LANES), 1), 1.0, 0.0)
    sums = jnp.dot(parts, upto.astype(jnp.bfloat16), preferred_element_type=jnp.float32)
    n = counts.shape[0]
    inside = sums[:n] + 256.0 * sums[n : 2 * n] + 65536.0 * sums[2 * n :]
    totals = jnp.broadcast_to(jnp.sum(counts, axis=1, keepdims=True), counts.shape)
    row_ids = iota(counts.shape, 0)
    for r in range(n - 1):
        inside = inside + jnp.where(row_ids > r, totals[r : r + 1], 0.0)
    return inside


def shade_kernel(mine, theirs, core_ref, ranks, bins, gx_ref, gy_ref, out_ref, done, sems):
    first = core_ref[0] == 0
    a, b = mine[...], theirs[...]
    lower = jnp.where(first, a, b)
    upper = jnp.where(first, b, a)
    span = lower[:, HALF:] + upper[:, HALF:]
    scale = zfactor / (8.0 * span)
    parts = [lower[:, i * LANES : (i + 1) * LANES] for i in range(4)]
    parts += [upper[:, i * LANES : (i + 1) * LANES] for i in range(4)]
    cumulative = prefix_sums(jnp.concatenate(parts, axis=0)).astype(jnp.int32)
    table = jnp.clip(
        (cumulative - ranks[0]).astype(jnp.float32)
        / jnp.full(cumulative.shape, ranks[1] - ranks[0]).astype(jnp.float32),
        0.0,
        1.0,
    )
    steps = jnp.floor(table * STEPS + 0.5).astype(jnp.int32)
    words = steps[:4] | (steps[4:] << 16)

    rows, width = bins.shape
    tables = [jnp.broadcast_to(words[r : r + 1], (rows, LANES)) for r in range(4)]
    pieces = sems.shape[0]
    piece = width // pieces
    copies = []
    for c in range(width // LANES):
        cols = slice(c * LANES, (c + 1) * LANES)
        code = bins[:, cols]
        low = code & (LANES - 1)
        w = [jnp.take_along_axis(t, low, axis=1, mode="promise_in_bounds") for t in tables]
        odd = (code & 128) != 0
        word = jnp.where((code & 256) != 0, jnp.where(odd, w[3], w[2]), jnp.where(odd, w[1], w[0]))
        stretch = ((word >> ((code >> 5) & 16)) & 65535).astype(jnp.float32)
        gx = gx_ref[:, cols] * scale
        gy = gy_ref[:, cols] * scale
        light = (cos_zenith - (sin_zenith * light_y) * (gy - gx)) * lax.rsqrt(
            1.0 + gx * gx + gy * gy
        )
        done[:, cols] = stretch * (0.5 / STEPS + jnp.maximum(light, 0.0) * (1.0 / STEPS))
        if (c + 1) * LANES % piece == 0:
            n = len(copies)
            span_cols = slice(n * piece, (n + 1) * piece)
            copies.append(
                pltpu.make_async_copy(done.at[:, span_cols], out_ref.at[:, span_cols], sems.at[n])
            )
            copies[-1].start()
    for copy in copies:
        copy.wait()


def shade(mine, theirs, core, ranks, bins, gx, gy):
    return pl.pallas_call(
        shade_kernel,
        out_shape=jax.ShapeDtypeStruct(gx.shape, jnp.float32),
        in_specs=[VMEM_SPEC, VMEM_SPEC, SMEM_SPEC, SMEM_SPEC, VMEM_SPEC, VMEM_SPEC, VMEM_SPEC],
        out_specs=pl.BlockSpec(memory_space=pl.ANY),
        scratch_shapes=[
            pltpu.VMEM(gx.shape, jnp.float32),
            pltpu.SemaphoreType.DMA((8,)),
        ],
        name="shade",
    )(mine, theirs, core, ranks, bins, gx, gy)


def body(elevation, ranks):
    size = lax.axis_size("row")
    core = lax.axis_index("row") & 1
    core = core.astype(jnp.int32).reshape(1)
    partner = [(i, i ^ 1) for i in range(size)]
    chips = size // 2
    begin = chips * 11 // 16
    order = [(i + begin) % chips for i in range(chips)]
    same_core = [[2 * i + c for i in order] for c in range(2)]
    local = in_vmem(elevation)
    keep, send = count(local, core)
    received = lax.ppermute(send, "row", partner)
    spread = join(in_vmem(keep), in_vmem(received), chips)
    everyone = lax.all_to_all(spread, "row", 0, 0, axis_index_groups=same_core, tiled=True)

    above = lax.ppermute(elevation[-4:], "row", [(i, i + 1) for i in range(size - 1)])
    below = lax.ppermute(elevation[:4], "row", [(i + 1, i) for i in range(size - 1)])
    gx, gy, bins = gradients(in_vmem(above), local, in_vmem(below))

    mine = gather(in_vmem(everyone))
    theirs = lax.ppermute(mine, "row", partner)
    return shade(
        in_vmem(mine), in_vmem(theirs), core, ranks, in_vmem(bins), in_vmem(gx), in_vmem(gy)
    )


def solution(mesh):
    whole = P(("groups", "row"), None)
    mapped = jax.shard_map(
        body, mesh=mesh, in_specs=(whole, P("groups")), out_specs=whole, check_vma=False
    )

    def run(elevation, bin_index, ranks):
        return mapped(elevation, ranks)

    return run
```

```python
import jax
import jax.numpy as jnp
from jax import lax
from jax.experimental import pallas as pl
from jax.experimental.pallas import tpu as pltpu
from jax.sharding import PartitionSpec as P

BINS = 1024
HALF = BINS // 2
LANES = 128
LOW = 32
WIRE = HALF + LANES

zfactor = 200.0
cos_zenith = 0.70710678
sin_zenith = 0.70710678
light_y = 0.70710678
HIGHEST = lax.Precision.HIGHEST
HOT = jnp.float8_e4m3fn
STEPS = 65535.0


def bin_of(height):
    return jnp.clip(jnp.floor(height * 0.5), 0.0, BINS - 1.0)


def iota(shape, dim):
    return lax.broadcasted_iota(jnp.int32, shape, dim)


def in_vmem(x):
    return pltpu.with_memory_space_constraint(x, pltpu.VMEM)


def count_kernel(heights, core_ref, keep_ref, send_ref, upper, lower):
    rows, width = heights.shape
    high_count = BINS // LOW
    bins = bin_of(heights[...])
    up = jnp.floor(bins * (1.0 / LOW))
    upper[...] = up
    lower[...] = bins - up * LOW
    row_ids = iota((LOW, width), 0).astype(jnp.float32).astype(jnp.bfloat16)
    one = jnp.array(1, HOT)
    zero = jnp.array(0, HOT)

    def hot(digits, r):
        again = digits[pl.ds(r, LOW // 2, stride=0), :].astype(jnp.bfloat16)
        return jnp.where(jnp.concatenate([again, again], axis=0) == row_ids, one, zero)

    grid = jnp.zeros((high_count, LOW), jnp.float32)
    for r in range(rows):
        grid = grid + lax.dot_general(
            hot(upper, r),
            hot(lower, r),
            (((1,), (1,)), ((), ())),
            preferred_element_type=jnp.float32,
        )
    spread = (iota((LOW, LANES), 1) % LOW == iota((LOW, LANES), 0)).astype(jnp.float32)
    tiled = jnp.dot(grid, spread, precision=HIGHEST, preferred_element_type=jnp.float32)
    quarter = iota((high_count, LANES), 1) // LOW == iota((high_count, LANES), 0) % 4
    fold = (iota((8, high_count), 1) // 4 == iota((8, high_count), 0)).astype(jnp.float32)
    flat = jnp.dot(
        fold, jnp.where(quarter, tiled, 0.0), precision=HIGHEST, preferred_element_type=jnp.float32
    )
    highest = jnp.max(heights[...])
    neg_lowest = -jnp.min(heights[...])
    first = core_ref[0] == 0
    for i in range(4):
        cols = slice(i * LANES, (i + 1) * LANES)
        keep_ref[:, cols] = jnp.where(first, flat[i : i + 1], flat[4 + i : 5 + i])
        send_ref[:, cols] = jnp.where(first, flat[4 + i : 5 + i], flat[i : i + 1])
    keep_ref[:, HALF:] = jnp.full((1, LANES), jnp.where(first, highest, neg_lowest))
    send_ref[:, HALF:] = jnp.full((1, LANES), jnp.where(first, neg_lowest, highest))


VMEM_SPEC = pl.BlockSpec(memory_space=pltpu.VMEM)
SMALL = pltpu.CompilerParams(vmem_limit_bytes=16 * 2**20)
SMEM_SPEC = pl.BlockSpec(memory_space=pltpu.SMEM)


def count(elevation, core):
    shape = pltpu.VMEM((1, WIRE), jnp.float32)
    return pl.pallas_call(
        count_kernel,
        out_shape=(shape, shape),
        in_specs=[VMEM_SPEC, SMEM_SPEC],
        out_specs=(VMEM_SPEC,) * 2,
        scratch_shapes=[pltpu.VMEM(elevation.shape, jnp.float32)] * 2,
        name="count",
        compiler_params=SMALL,
    )(elevation, core)


def join_kernel(a_ref, b_ref, c_ref, d_ref, out_ref):
    a, b, c, d = a_ref[...], b_ref[...], c_ref[...], d_ref[...]
    added = (a + b) + (c + d)
    largest = jnp.maximum(jnp.maximum(a, b), jnp.maximum(c, d))
    joined = jnp.where(iota(a.shape, 1) < HALF, added, largest)
    out_ref[...] = jnp.broadcast_to(joined[None], out_ref.shape)


def join(a, b, c, d, copies):
    return pl.pallas_call(
        join_kernel,
        out_shape=pltpu.VMEM((copies, *a.shape), jnp.float32),
        in_specs=[VMEM_SPEC] * 4,
        out_specs=VMEM_SPEC,
        name="join",
        compiler_params=SMALL,
    )(a, b, c, d)


def gather_kernel(x_ref, out_ref):
    x = x_ref[...]
    out_ref[:, :HALF] = jnp.sum(x[:, :, :HALF], axis=0)
    out_ref[:, HALF:] = jnp.max(x[:, :, HALF:], axis=0)


def gather(everyone):
    return pl.pallas_call(
        gather_kernel,
        out_shape=pltpu.VMEM((1, WIRE), jnp.float32),
        in_specs=[VMEM_SPEC],
        out_specs=VMEM_SPEC,
        name="gather",
        compiler_params=SMALL,
    )(everyone)


def gradient_kernel(above, middle, below, ranks, gx_ref, gy_ref, bin_ref, rank_ref, wide):
    rank_ref[:1] = jnp.full((1, LANES), ranks[0])
    rank_ref[1:] = jnp.full((1, LANES), ranks[1] - ranks[0])
    rows, width = middle.shape
    halo = above.shape[0]
    edge = jnp.zeros((rows + 2 * halo, LANES), jnp.float32)
    wide[:, :LANES] = edge
    wide[:, LANES + width :] = edge
    wide[:halo, LANES : LANES + width] = above[...]
    wide[halo : halo + rows, LANES : LANES + width] = middle[...]
    wide[halo + rows :, LANES : LANES + width] = below[...]
    chunk = 4 * LANES
    tall = rows + 2 * halo
    for c in range(0, width, chunk):
        x = wide[:, LANES + c : LANES + c + chunk]
        for _ in range(7):
            x = x + pltpu.roll(x, tall - 1, 0)
        wide[:, LANES + c : LANES + c + chunk] = x * (1.0 / 4096)
    for c in range(0, width, chunk):
        x = wide[:, c : c + chunk + 2 * LANES]
        across = x.shape[1]

        def moved(k):
            return pltpu.roll(x, (-k) % across, 1)[:, LANES : LANES + chunk]

        right = [moved(k) for k in range(1, 5)]
        left = [moved(-k) for k in range(1, 5)]
        d1, d2, d3, d4 = (r - l for r, l in zip(right, left))
        s1, s2, s3, s4 = (r + l for r, l in zip(right, left))
        east = d4 + 6.0 * d3 + 14.0 * (d2 + d1)
        both = s4 + 8.0 * s3 + 28.0 * s2 + 56.0 * s1 + 70.0 * x[:, LANES : LANES + chunk]
        gx = east + pltpu.roll(east, tall - 1, 0)
        gy = pltpu.roll(both, tall - 1, 0) - both
        bin_ref[:, c : c + chunk] = bin_of(middle[:, c : c + chunk]).astype(jnp.int32)
        gx_ref[:, c : c + chunk] = gx[:rows]
        gy_ref[:, c : c + chunk] = gy[:rows]


def gradients(above, middle, below, ranks):
    rows, width = middle.shape
    shape = pltpu.VMEM(middle.shape, jnp.float32)
    return pl.pallas_call(
        gradient_kernel,
        out_shape=(
            shape,
            shape,
            pltpu.VMEM(middle.shape, jnp.int32),
            pltpu.VMEM((2, LANES), jnp.int32),
        ),
        in_specs=[VMEM_SPEC] * 3 + [SMEM_SPEC],
        out_specs=(VMEM_SPEC,) * 4,
        scratch_shapes=[
            pltpu.VMEM((rows + 2 * above.shape[0], width + 2 * LANES), jnp.float32)
        ],
        name="gradients",
        compiler_params=SMALL,
    )(above, middle, below, ranks)


def prefix_sums(counts):
    whole = counts.astype(jnp.int32)
    parts = [(whole >> shift) & 255 for shift in (0, 8, 16)]
    parts = jnp.concatenate(parts, axis=0).astype(jnp.float32).astype(jnp.bfloat16)
    upto = jnp.where(iota((LANES, LANES), 0) <= iota((LANES, LANES), 1), 1.0, 0.0)
    sums = jnp.dot(parts, upto.astype(jnp.bfloat16), preferred_element_type=jnp.float32)
    n = counts.shape[0]
    inside = sums[:n] + 256.0 * sums[n : 2 * n] + 65536.0 * sums[2 * n :]
    totals = jnp.broadcast_to(jnp.sum(counts, axis=1, keepdims=True), counts.shape)
    row_ids = iota(counts.shape, 0)
    for r in range(n - 1):
        inside = inside + jnp.where(row_ids > r, totals[r : r + 1], 0.0)
    return inside


def shade_kernel(mine, theirs, core_ref, limits, bins, gx_ref, gy_ref, out_ref, done, sems):
    first = core_ref[0] == 0
    a, b = mine[...], theirs[...]
    lower = jnp.where(first, a, b)
    upper = jnp.where(first, b, a)
    span = lower[:, HALF:] + upper[:, HALF:]
    scale = zfactor / (8.0 * span)
    parts = [lower[:, i * LANES : (i + 1) * LANES] for i in range(4)]
    parts += [upper[:, i * LANES : (i + 1) * LANES] for i in range(4)]
    cumulative = prefix_sums(jnp.concatenate(parts, axis=0)).astype(jnp.int32)
    table = jnp.clip(
        (cumulative - limits[:1]).astype(jnp.float32) / limits[1:].astype(jnp.float32),
        0.0,
        1.0,
    )
    steps = jnp.floor(table * STEPS + 0.5).astype(jnp.int32)
    words = steps[:4] | (steps[4:] << 16)

    rows, width = bins.shape
    tables = [jnp.broadcast_to(words[r : r + 1], (rows, LANES)) for r in range(4)]
    pieces = sems.shape[0]
    piece = width // pieces
    copies = []
    for c in range(width // LANES):
        cols = slice(c * LANES, (c + 1) * LANES)
        code = bins[:, cols]
        low = code & (LANES - 1)
        w = [jnp.take_along_axis(t, low, axis=1, mode="promise_in_bounds") for t in tables]
        odd = (code & 128) != 0
        word = jnp.where((code & 256) != 0, jnp.where(odd, w[3], w[2]), jnp.where(odd, w[1], w[0]))
        stretch = ((word >> ((code >> 5) & 16)) & 65535).astype(jnp.float32)
        gx = gx_ref[:, cols] * scale
        gy = gy_ref[:, cols] * scale
        light = (cos_zenith - (sin_zenith * light_y) * (gy - gx)) * lax.rsqrt(
            1.0 + gx * gx + gy * gy
        )
        done[:, cols] = stretch * (0.5 / STEPS + jnp.maximum(light, 0.0) * (1.0 / STEPS))
        if (c + 1) * LANES % piece == 0:
            n = len(copies)
            span_cols = slice(n * piece, (n + 1) * piece)
            copies.append(
                pltpu.make_async_copy(done.at[:, span_cols], out_ref.at[:, span_cols], sems.at[n])
            )
            copies[-1].start()
    for copy in copies:
        copy.wait()


def shade(mine, theirs, core, limits, bins, gx, gy):
    return pl.pallas_call(
        shade_kernel,
        out_shape=jax.ShapeDtypeStruct(gx.shape, jnp.float32),
        in_specs=[VMEM_SPEC, VMEM_SPEC, SMEM_SPEC, VMEM_SPEC, VMEM_SPEC, VMEM_SPEC, VMEM_SPEC],
        out_specs=pl.BlockSpec(memory_space=pl.ANY),
        scratch_shapes=[
            pltpu.VMEM(gx.shape, jnp.float32),
            pltpu.SemaphoreType.DMA((16,)),
        ],
        name="shade",
        compiler_params=SMALL,
    )(mine, theirs, core, limits, bins, gx, gy)


def body(elevation, ranks):
    size = lax.axis_size("row")
    core = lax.axis_index("row") & 1
    core = core.astype(jnp.int32).reshape(1)
    partner = [(i, i ^ 1) for i in range(size)]
    blocks = size // 4
    begin = blocks * 3 // 4
    order = [(i + begin) % blocks for i in range(blocks)]
    alike = [[4 * i + place for i in order] for place in range(4)]
    local = in_vmem(elevation)
    keep, send = count(local, core)
    received = lax.ppermute(send, "row", partner)
    beside = lax.ppermute(keep, "row", [(i, i ^ 2) for i in range(size)])
    across = lax.ppermute(send, "row", [(i, i ^ 3) for i in range(size)])
    spread = join(
        in_vmem(keep), in_vmem(received), in_vmem(beside), in_vmem(across), blocks
    )
    everyone = lax.all_to_all(spread, "row", 0, 0, axis_index_groups=alike, tiled=True)

    above = lax.ppermute(elevation[-4:], "row", [(i, i + 1) for i in range(size - 1)])
    below = lax.ppermute(elevation[:4], "row", [(i + 1, i) for i in range(size - 1)])
    gx, gy, bins, limits = gradients(
        in_vmem(above), local, in_vmem(below), ranks
    )

    mine = gather(in_vmem(everyone))
    theirs = lax.ppermute(mine, "row", partner)
    return shade(
        in_vmem(mine), in_vmem(theirs), core, in_vmem(limits), in_vmem(bins), in_vmem(gx), in_vmem(gy)
    )


def solution(mesh):
    whole = P(("groups", "row"), None)
    mapped = jax.shard_map(
        body, mesh=mesh, in_specs=(whole, P("groups")), out_specs=whole, check_vma=False
    )

    def run(elevation, bin_index, ranks):
        return mapped(elevation, ranks)

    return run
```

```python
import jax
import jax.numpy as jnp
from jax import lax
from jax.experimental import pallas as pl
from jax.experimental.pallas import tpu as pltpu
from jax.sharding import PartitionSpec as P

BINS = 1024
HALF = BINS // 2
LANES = 128
LOW = 32
WIRE = HALF + LANES

zfactor = 200.0
cos_zenith = 0.70710678
sin_zenith = 0.70710678
light_y = 0.70710678
HIGHEST = lax.Precision.HIGHEST
HOT = jnp.float8_e4m3fn
STEPS = 65535.0


def bin_of(height):
    return jnp.clip(jnp.floor(height * 0.5), 0.0, BINS - 1.0)


def iota(shape, dim):
    return lax.broadcasted_iota(jnp.int32, shape, dim)


def in_vmem(x):
    return pltpu.with_memory_space_constraint(x, pltpu.VMEM)


def count_kernel(heights, keep_ref, send_ref, upper, lower):
    rows, width = heights.shape
    high_count = BINS // LOW
    bins = bin_of(heights[...])
    up = jnp.floor(bins * (1.0 / LOW))
    upper[...] = up
    lower[...] = bins - up * LOW
    row_ids = iota((LOW, width), 0).astype(jnp.float32).astype(jnp.bfloat16)
    one = jnp.array(1, HOT)
    zero = jnp.array(0, HOT)

    def hot(digits, r):
        again = digits[pl.ds(r, LOW // 2, stride=0), :].astype(jnp.bfloat16)
        return jnp.where(jnp.concatenate([again, again], axis=0) == row_ids, one, zero)

    grid = jnp.zeros((high_count, LOW), jnp.float32)
    for r in range(rows):
        grid = grid + lax.dot_general(
            hot(upper, r),
            hot(lower, r),
            (((1,), (1,)), ((), ())),
            preferred_element_type=jnp.float32,
        )
    spread = (iota((LOW, LANES), 1) % LOW == iota((LOW, LANES), 0)).astype(jnp.float32)
    tiled = jnp.dot(grid, spread, precision=HIGHEST, preferred_element_type=jnp.float32)
    quarter = iota((high_count, LANES), 1) // LOW == iota((high_count, LANES), 0) % 4
    fold = (iota((8, high_count), 1) // 4 == iota((8, high_count), 0)).astype(jnp.float32)
    flat = jnp.dot(
        fold, jnp.where(quarter, tiled, 0.0), precision=HIGHEST, preferred_element_type=jnp.float32
    )
    highest = jnp.max(heights[...])
    neg_lowest = -jnp.min(heights[...])
    first = lax.axis_index("row") & 1 == 0
    for i in range(4):
        cols = slice(i * LANES, (i + 1) * LANES)
        keep_ref[:, cols] = jnp.where(first, flat[i : i + 1], flat[4 + i : 5 + i])
        send_ref[:, cols] = jnp.where(first, flat[4 + i : 5 + i], flat[i : i + 1])
    keep_ref[:, HALF:] = jnp.full((1, LANES), jnp.where(first, highest, neg_lowest))
    send_ref[:, HALF:] = jnp.full((1, LANES), jnp.where(first, neg_lowest, highest))


VMEM_SPEC = pl.BlockSpec(memory_space=pltpu.VMEM)
SMALL = pltpu.CompilerParams(vmem_limit_bytes=16 * 2**20)


def count(elevation):
    shape = pltpu.VMEM((1, WIRE), jnp.float32)
    return pl.pallas_call(
        count_kernel,
        out_shape=(shape, shape),
        in_specs=[VMEM_SPEC],
        out_specs=(VMEM_SPEC,) * 2,
        scratch_shapes=[pltpu.VMEM(elevation.shape, jnp.float32)] * 2,
        name="count",
        compiler_params=SMALL,
    )(elevation)


def join_kernel(a_ref, b_ref, c_ref, d_ref, out_ref):
    a, b, c, d = a_ref[...], b_ref[...], c_ref[...], d_ref[...]
    added = (a + b) + (c + d)
    largest = jnp.maximum(jnp.maximum(a, b), jnp.maximum(c, d))
    joined = jnp.where(iota(a.shape, 1) < HALF, added, largest)
    out_ref[...] = jnp.broadcast_to(joined[None], out_ref.shape)


def join(a, b, c, d, copies):
    return pl.pallas_call(
        join_kernel,
        out_shape=pltpu.VMEM((copies, *a.shape), jnp.float32),
        in_specs=[VMEM_SPEC] * 4,
        out_specs=VMEM_SPEC,
        name="join",
        compiler_params=SMALL,
    )(a, b, c, d)


def gather_kernel(x_ref, out_ref):
    x = x_ref[...]
    out_ref[:, :HALF] = jnp.sum(x[:, :, :HALF], axis=0)
    out_ref[:, HALF:] = jnp.max(x[:, :, HALF:], axis=0)


def gather(everyone):
    return pl.pallas_call(
        gather_kernel,
        out_shape=pltpu.VMEM((1, WIRE), jnp.float32),
        in_specs=[VMEM_SPEC],
        out_specs=VMEM_SPEC,
        name="gather",
        compiler_params=SMALL,
    )(everyone)


def gradient_kernel(above, middle, below, ranks, gx_ref, gy_ref, bin_ref, rank_ref, wide):
    low, high = ranks[:, :1], ranks[:, 1:]
    rank_ref[:1] = jnp.broadcast_to(low, (1, LANES))
    rank_ref[1:] = jnp.broadcast_to(high - low, (1, LANES))
    rows, width = middle.shape
    halo = above.shape[0]
    edge = jnp.zeros((rows + 2 * halo, LANES), jnp.float32)
    wide[:, :LANES] = edge
    wide[:, LANES + width :] = edge
    wide[:halo, LANES : LANES + width] = above[...]
    wide[halo : halo + rows, LANES : LANES + width] = middle[...]
    wide[halo + rows :, LANES : LANES + width] = below[...]
    chunk = 4 * LANES
    tall = rows + 2 * halo
    for c in range(0, width, chunk):
        x = wide[:, LANES + c : LANES + c + chunk]
        for _ in range(7):
            x = x + pltpu.roll(x, tall - 1, 0)
        wide[:, LANES + c : LANES + c + chunk] = x * (1.0 / 4096)
    for c in range(0, width, chunk):
        x = wide[:, c : c + chunk + 2 * LANES]
        across = x.shape[1]

        def moved(k):
            return pltpu.roll(x, (-k) % across, 1)[:, LANES : LANES + chunk]

        right = [moved(k) for k in range(1, 5)]
        left = [moved(-k) for k in range(1, 5)]
        d1, d2, d3, d4 = (r - l for r, l in zip(right, left))
        s1, s2, s3, s4 = (r + l for r, l in zip(right, left))
        east = d4 + 6.0 * d3 + 14.0 * (d2 + d1)
        both = s4 + 8.0 * s3 + 28.0 * s2 + 56.0 * s1 + 70.0 * x[:, LANES : LANES + chunk]
        gx = east + pltpu.roll(east, tall - 1, 0)
        gy = pltpu.roll(both, tall - 1, 0) - both
        bin_ref[:, c : c + chunk] = bin_of(middle[:, c : c + chunk]).astype(jnp.int32)
        gx_ref[:, c : c + chunk] = gx[:rows]
        gy_ref[:, c : c + chunk] = gy[:rows]


def gradients(above, middle, below, ranks):
    rows, width = middle.shape
    shape = pltpu.VMEM(middle.shape, jnp.float32)
    return pl.pallas_call(
        gradient_kernel,
        out_shape=(
            shape,
            shape,
            pltpu.VMEM(middle.shape, jnp.int32),
            pltpu.VMEM((2, LANES), jnp.int32),
        ),
        in_specs=[VMEM_SPEC] * 4,
        out_specs=(VMEM_SPEC,) * 4,
        scratch_shapes=[
            pltpu.VMEM((rows + 2 * above.shape[0], width + 2 * LANES), jnp.float32)
        ],
        name="gradients",
        compiler_params=SMALL,
    )(above, middle, below, ranks)


def prefix_sums(counts):
    whole = counts.astype(jnp.int32)
    parts = [(whole >> shift) & 255 for shift in (0, 8, 16)]
    parts = jnp.concatenate(parts, axis=0).astype(jnp.float32).astype(jnp.bfloat16)
    upto = jnp.where(iota((LANES, LANES), 0) <= iota((LANES, LANES), 1), 1.0, 0.0)
    sums = jnp.dot(parts, upto.astype(jnp.bfloat16), preferred_element_type=jnp.float32)
    n = counts.shape[0]
    inside = sums[:n] + 256.0 * sums[n : 2 * n] + 65536.0 * sums[2 * n :]
    totals = jnp.broadcast_to(jnp.sum(counts, axis=1, keepdims=True), counts.shape)
    row_ids = iota(counts.shape, 0)
    for r in range(n - 1):
        inside = inside + jnp.where(row_ids > r, totals[r : r + 1], 0.0)
    return inside


def shade_kernel(mine, theirs, limits, bins, gx_ref, gy_ref, out_ref, done, sems):
    first = lax.axis_index("row") & 1 == 0
    a, b = mine[...], theirs[...]
    lower = jnp.where(first, a, b)
    upper = jnp.where(first, b, a)
    span = lower[:, HALF:] + upper[:, HALF:]
    scale = zfactor / (8.0 * span)
    parts = [lower[:, i * LANES : (i + 1) * LANES] for i in range(4)]
    parts += [upper[:, i * LANES : (i + 1) * LANES] for i in range(4)]
    cumulative = prefix_sums(jnp.concatenate(parts, axis=0)).astype(jnp.int32)
    table = jnp.clip(
        (cumulative - limits[:1]).astype(jnp.float32) / limits[1:].astype(jnp.float32),
        0.0,
        1.0,
    )
    steps = jnp.floor(table * STEPS + 0.5).astype(jnp.int32)
    words = steps[:4] | (steps[4:] << 16)

    rows, width = bins.shape
    tables = [jnp.broadcast_to(words[r : r + 1], (rows, LANES)) for r in range(4)]
    pieces = sems.shape[0]
    piece = width // pieces
    copies = []
    for c in range(width // LANES):
        cols = slice(c * LANES, (c + 1) * LANES)
        code = bins[:, cols]
        low = code & (LANES - 1)
        w = [jnp.take_along_axis(t, low, axis=1, mode="promise_in_bounds") for t in tables]
        odd = (code & 128) != 0
        word = jnp.where((code & 256) != 0, jnp.where(odd, w[3], w[2]), jnp.where(odd, w[1], w[0]))
        stretch = ((word >> ((code >> 5) & 16)) & 65535).astype(jnp.float32)
        gx = gx_ref[:, cols] * scale
        gy = gy_ref[:, cols] * scale
        light = (cos_zenith - (sin_zenith * light_y) * (gy - gx)) * lax.rsqrt(
            1.0 + gx * gx + gy * gy
        )
        done[:, cols] = stretch * (0.5 / STEPS + jnp.maximum(light, 0.0) * (1.0 / STEPS))
        if (c + 1) * LANES % piece == 0:
            n = len(copies)
            span_cols = slice(n * piece, (n + 1) * piece)
            copies.append(
                pltpu.make_async_copy(done.at[:, span_cols], out_ref.at[:, span_cols], sems.at[n])
            )
            copies[-1].start()
    for copy in copies:
        copy.wait()


def shade(mine, theirs, limits, bins, gx, gy):
    return pl.pallas_call(
        shade_kernel,
        out_shape=jax.ShapeDtypeStruct(gx.shape, jnp.float32),
        in_specs=[VMEM_SPEC] * 6,
        out_specs=pl.BlockSpec(memory_space=pl.ANY),
        scratch_shapes=[
            pltpu.VMEM(gx.shape, jnp.float32),
            pltpu.SemaphoreType.DMA((16,)),
        ],
        name="shade",
        compiler_params=SMALL,
    )(mine, theirs, limits, bins, gx, gy)


def body(elevation, ranks):
    size = lax.axis_size("row")
    partner = [(i, i ^ 1) for i in range(size)]
    blocks = size // 4
    begin = blocks * 3 // 4
    order = [(i + begin) % blocks for i in range(blocks)]
    alike = [[4 * i + place for i in order] for place in range(4)]
    local = in_vmem(elevation)
    keep, send = count(local)
    received = lax.ppermute(send, "row", partner)
    beside = lax.ppermute(keep, "row", [(i, i ^ 2) for i in range(size)])
    across = lax.ppermute(send, "row", [(i, i ^ 3) for i in range(size)])
    spread = join(
        in_vmem(keep), in_vmem(received), in_vmem(beside), in_vmem(across), blocks
    )
    everyone = lax.all_to_all(spread, "row", 0, 0, axis_index_groups=alike, tiled=True)

    above = lax.ppermute(elevation[-4:], "row", [(i, i + 1) for i in range(size - 1)])
    below = lax.ppermute(elevation[:4], "row", [(i + 1, i) for i in range(size - 1)])
    gx, gy, bins, limits = gradients(
        in_vmem(above), local, in_vmem(below), in_vmem(ranks.reshape(1, 2))
    )

    mine = gather(in_vmem(everyone))
    theirs = lax.ppermute(mine, "row", partner)
    return shade(
        in_vmem(mine), in_vmem(theirs), in_vmem(limits), in_vmem(bins), in_vmem(gx), in_vmem(gy)
    )


def solution(mesh):
    whole = P(("groups", "row"), None)
    mapped = jax.shard_map(
        body, mesh=mesh, in_specs=(whole, P("groups")), out_specs=whole, check_vma=False
    )

    def run(elevation, bin_index, ranks):
        return mapped(elevation, ranks)

    return run
```

```python
import jax
import jax.numpy as jnp
from jax import lax
from jax.experimental import pallas as pl
from jax.experimental.pallas import tpu as pltpu
from jax.sharding import PartitionSpec as P

BINS = 1024
HALF = BINS // 2
LANES = 128
LOW = 32
WIRE = HALF + LANES

zfactor = 200.0
cos_zenith = 0.70710678
sin_zenith = 0.70710678
light_y = 0.70710678
HOT = jnp.float8_e4m3fn
STEPS = 65535.0


def bin_of(height):
    return jnp.clip(jnp.floor(height * 0.5), 0.0, BINS - 1.0)


def iota(shape, dim):
    return lax.broadcasted_iota(jnp.int32, shape, dim)


def in_vmem(x):
    return pltpu.with_memory_space_constraint(x, pltpu.VMEM)


def count_kernel(source, keep_ref, send_ref, heights, upper, lower, sems):
    rows, width = heights.shape
    part = width // sems.shape[0]
    copies = []
    for i in range(sems.shape[0]):
        some = slice(i * part, (i + 1) * part)
        copies.append(
            pltpu.make_async_copy(source.at[:, some], heights.at[:, some], sems.at[i])
        )
        copies[-1].start()
    for copy in copies:
        copy.wait()
    high_count = BINS // LOW
    bins = bin_of(heights[...])
    up = jnp.floor(bins * (1.0 / LOW))
    upper[...] = up
    lower[...] = bins - up * LOW
    row_ids = iota((LOW, width), 0).astype(jnp.float32).astype(jnp.bfloat16)
    one = jnp.array(1, HOT)
    zero = jnp.array(0, HOT)

    def hot(digits, r):
        again = digits[pl.ds(r, LOW // 2, stride=0), :].astype(jnp.bfloat16)
        return jnp.where(jnp.concatenate([again, again], axis=0) == row_ids, one, zero)

    grid = jnp.zeros((high_count, LOW), jnp.float32)
    for r in range(rows):
        grid = grid + lax.dot_general(
            hot(upper, r),
            hot(lower, r),
            (((1,), (1,)), ((), ())),
            preferred_element_type=jnp.float32,
        )
    tiled = jnp.concatenate([grid] * (LANES // LOW), axis=1)
    quarter = iota((high_count, LANES), 1) // LOW == iota((high_count, LANES), 0) % 4
    flat = jnp.where(quarter, tiled, 0.0)
    flat = flat + pltpu.roll(flat, high_count - 1, 0)
    flat = flat + pltpu.roll(flat, high_count - 2, 0)
    highest = jnp.max(heights[...])
    neg_lowest = -jnp.min(heights[...])
    first = lax.axis_index("row") & 1 == 0
    for i in range(4):
        cols = slice(i * LANES, (i + 1) * LANES)
        lower_row, upper_row = (flat[j : j + 1] for j in (4 * i, 4 * i + 16))
        keep_ref[:, cols] = jnp.where(first, lower_row, upper_row)
        send_ref[:, cols] = jnp.where(first, upper_row, lower_row)
    keep_ref[:, HALF:] = jnp.full((1, LANES), jnp.where(first, highest, neg_lowest))
    send_ref[:, HALF:] = jnp.full((1, LANES), jnp.where(first, neg_lowest, highest))


VMEM_SPEC = pl.BlockSpec(memory_space=pltpu.VMEM)
SMALL = pltpu.CompilerParams(vmem_limit_bytes=16 * 2**20)


def count(elevation):
    shape = pltpu.VMEM((1, WIRE), jnp.float32)
    return pl.pallas_call(
        count_kernel,
        out_shape=(shape, shape, pltpu.VMEM(elevation.shape, jnp.float32)),
        in_specs=[pl.BlockSpec(memory_space=pltpu.HBM)],
        out_specs=(VMEM_SPEC,) * 3,
        scratch_shapes=[pltpu.VMEM(elevation.shape, jnp.float32)] * 2
        + [pltpu.SemaphoreType.DMA((4,))],
        name="count",
        compiler_params=SMALL,
    )(elevation)


def join_kernel(a_ref, b_ref, c_ref, d_ref, out_ref):
    a, b, c, d = a_ref[...], b_ref[...], c_ref[...], d_ref[...]
    added = (a + b) + (c + d)
    largest = jnp.maximum(jnp.maximum(a, b), jnp.maximum(c, d))
    joined = jnp.where(iota(a.shape, 1) < HALF, added, largest)
    out_ref[...] = jnp.broadcast_to(joined[None], out_ref.shape)


def join(a, b, c, d, copies):
    return pl.pallas_call(
        join_kernel,
        out_shape=pltpu.VMEM((copies, *a.shape), jnp.float32),
        in_specs=[VMEM_SPEC] * 4,
        out_specs=VMEM_SPEC,
        name="join",
        compiler_params=SMALL,
    )(a, b, c, d)


def gather_kernel(x_ref, out_ref):
    x = x_ref[...]
    out_ref[:, :HALF] = jnp.sum(x[:, :, :HALF], axis=0)
    out_ref[:, HALF:] = jnp.max(x[:, :, HALF:], axis=0)


def gather(everyone):
    return pl.pallas_call(
        gather_kernel,
        out_shape=pltpu.VMEM((1, WIRE), jnp.float32),
        in_specs=[VMEM_SPEC],
        out_specs=VMEM_SPEC,
        name="gather",
        compiler_params=SMALL,
    )(everyone)


def gradient_kernel(above, middle, below, ranks, gx_ref, gy_ref, bin_ref, rank_ref, wide):
    low, high = ranks[:, :1], ranks[:, 1:]
    rank_ref[:1] = jnp.broadcast_to(low, (1, LANES))
    rank_ref[1:] = jnp.broadcast_to(high - low, (1, LANES))
    rows, width = middle.shape
    halo = above.shape[0]
    edge = jnp.zeros((rows + 2 * halo, LANES), jnp.float32)
    wide[:, :LANES] = edge
    wide[:, LANES + width :] = edge
    wide[:halo, LANES : LANES + width] = above[...]
    wide[halo : halo + rows, LANES : LANES + width] = middle[...]
    wide[halo + rows :, LANES : LANES + width] = below[...]
    chunk = 4 * LANES
    tall = rows + 2 * halo
    for c in range(0, width, chunk):
        x = wide[:, LANES + c : LANES + c + chunk]
        for _ in range(7):
            x = x + pltpu.roll(x, tall - 1, 0)
        wide[:, LANES + c : LANES + c + chunk] = x * (1.0 / 4096)
    for c in range(0, width, chunk):
        x = wide[:, c : c + chunk + 2 * LANES]
        across = x.shape[1]

        def moved(k):
            return pltpu.roll(x, (-k) % across, 1)[:, LANES : LANES + chunk]

        right = [moved(k) for k in range(1, 5)]
        left = [moved(-k) for k in range(1, 5)]
        d1, d2, d3, d4 = (r - l for r, l in zip(right, left))
        s1, s2, s3, s4 = (r + l for r, l in zip(right, left))
        east = d4 + 6.0 * d3 + 14.0 * (d2 + d1)
        both = s4 + 8.0 * s3 + 28.0 * s2 + 56.0 * s1 + 70.0 * x[:, LANES : LANES + chunk]
        gx = east + pltpu.roll(east, tall - 1, 0)
        gy = pltpu.roll(both, tall - 1, 0) - both
        bin_ref[:, c : c + chunk] = bin_of(middle[:, c : c + chunk]).astype(jnp.int32)
        gx_ref[:, c : c + chunk] = gx[:rows]
        gy_ref[:, c : c + chunk] = gy[:rows]


def gradients(above, middle, below, ranks):
    rows, width = middle.shape
    shape = pltpu.VMEM(middle.shape, jnp.float32)
    return pl.pallas_call(
        gradient_kernel,
        out_shape=(
            shape,
            shape,
            pltpu.VMEM(middle.shape, jnp.int32),
            pltpu.VMEM((2, LANES), jnp.int32),
        ),
        in_specs=[VMEM_SPEC] * 4,
        out_specs=(VMEM_SPEC,) * 4,
        scratch_shapes=[
            pltpu.VMEM((rows + 2 * above.shape[0], width + 2 * LANES), jnp.float32)
        ],
        name="gradients",
        compiler_params=SMALL,
    )(above, middle, below, ranks)


def prefix_sums(counts):
    whole = counts.astype(jnp.int32)
    parts = [(whole >> shift) & 255 for shift in (0, 8, 16)]
    parts = jnp.concatenate(parts, axis=0).astype(jnp.float32).astype(jnp.bfloat16)
    upto = jnp.where(iota((LANES, LANES), 0) <= iota((LANES, LANES), 1), 1.0, 0.0)
    sums = jnp.dot(parts, upto.astype(jnp.bfloat16), preferred_element_type=jnp.float32)
    n = counts.shape[0]
    inside = sums[:n] + 256.0 * sums[n : 2 * n] + 65536.0 * sums[2 * n :]
    totals = jnp.broadcast_to(jnp.sum(counts, axis=1, keepdims=True), counts.shape)
    row_ids = iota(counts.shape, 0)
    for r in range(n - 1):
        inside = inside + jnp.where(row_ids > r, totals[r : r + 1], 0.0)
    return inside


def shade_kernel(mine, theirs, limits, bins, gx_ref, gy_ref, out_ref, done, sems):
    first = lax.axis_index("row") & 1 == 0
    a, b = mine[...], theirs[...]
    lower = jnp.where(first, a, b)
    upper = jnp.where(first, b, a)
    span = lower[:, HALF:] + upper[:, HALF:]
    scale = zfactor / (8.0 * span)
    parts = [lower[:, i * LANES : (i + 1) * LANES] for i in range(4)]
    parts += [upper[:, i * LANES : (i + 1) * LANES] for i in range(4)]
    cumulative = prefix_sums(jnp.concatenate(parts, axis=0)).astype(jnp.int32)
    table = jnp.clip(
        (cumulative - limits[:1]).astype(jnp.float32) / limits[1:].astype(jnp.float32),
        0.0,
        1.0,
    )
    steps = jnp.floor(table * STEPS + 0.5).astype(jnp.int32)
    words = steps[:4] | (steps[4:] << 16)

    rows, width = bins.shape
    for c in range(width // LANES):
        cols = slice(c * LANES, (c + 1) * LANES)
        gx = gx_ref[:, cols] * scale
        gy = gy_ref[:, cols] * scale
        light = (cos_zenith - (sin_zenith * light_y) * (gy - gx)) * lax.rsqrt(
            1.0 + gx * gx + gy * gy
        )
        done[:, cols] = 0.5 / STEPS + jnp.maximum(light, 0.0) * (1.0 / STEPS)
    tables = [jnp.broadcast_to(words[r : r + 1], (rows, LANES)) for r in range(4)]
    pieces = sems.shape[0]
    piece = width // pieces
    copies = []
    for c in range(width // LANES):
        cols = slice(c * LANES, (c + 1) * LANES)
        code = bins[:, cols]
        low = code & (LANES - 1)
        w = [jnp.take_along_axis(t, low, axis=1, mode="promise_in_bounds") for t in tables]
        odd = (code & 128) != 0
        word = jnp.where((code & 256) != 0, jnp.where(odd, w[3], w[2]), jnp.where(odd, w[1], w[0]))
        stretch = ((word >> ((code >> 5) & 16)) & 65535).astype(jnp.float32)
        done[:, cols] = stretch * done[:, cols]
        if (c + 1) * LANES % piece == 0:
            n = len(copies)
            span_cols = slice(n * piece, (n + 1) * piece)
            copies.append(
                pltpu.make_async_copy(done.at[:, span_cols], out_ref.at[:, span_cols], sems.at[n])
            )
            copies[-1].start()
    for copy in copies:
        copy.wait()


def shade(mine, theirs, limits, bins, gx, gy):
    return pl.pallas_call(
        shade_kernel,
        out_shape=jax.ShapeDtypeStruct(gx.shape, jnp.float32),
        in_specs=[VMEM_SPEC] * 6,
        out_specs=pl.BlockSpec(memory_space=pl.ANY),
        scratch_shapes=[
            pltpu.VMEM(gx.shape, jnp.float32),
            pltpu.SemaphoreType.DMA((16,)),
        ],
        name="shade",
        compiler_params=SMALL,
    )(mine, theirs, limits, bins, gx, gy)


def body(elevation, ranks):
    size = lax.axis_size("row")
    partner = [(i, i ^ 1) for i in range(size)]
    blocks = size // 4
    begin = blocks * 3 // 4
    order = [(i + begin) % blocks for i in range(blocks)]
    alike = [[4 * i + place for i in order] for place in range(4)]
    keep, send, local = count(pltpu.with_memory_space_constraint(elevation, pltpu.HBM))
    received = lax.ppermute(send, "row", partner)
    beside = lax.ppermute(keep, "row", [(i, i ^ 2) for i in range(size)])
    across = lax.ppermute(send, "row", [(i, i ^ 3) for i in range(size)])
    spread = join(
        in_vmem(keep), in_vmem(received), in_vmem(beside), in_vmem(across), blocks
    )
    everyone = lax.all_to_all(spread, "row", 0, 0, axis_index_groups=alike, tiled=True)

    above = lax.ppermute(local[-4:], "row", [(i, i + 1) for i in range(size - 1)])
    below = lax.ppermute(local[:4], "row", [(i + 1, i) for i in range(size - 1)])
    gx, gy, bins, limits = gradients(
        in_vmem(above), in_vmem(local), in_vmem(below), in_vmem(ranks.reshape(1, 2))
    )

    mine = gather(in_vmem(everyone))
    theirs = lax.ppermute(mine, "row", partner)
    return shade(
        in_vmem(mine), in_vmem(theirs), in_vmem(limits), in_vmem(bins), in_vmem(gx), in_vmem(gy)
    )


def solution(mesh):
    whole = P(("groups", "row"), None)
    mapped = jax.shard_map(
        body, mesh=mesh, in_specs=(whole, P("groups")), out_specs=whole, check_vma=False
    )

    def run(elevation, bin_index, ranks):
        return mapped(elevation, ranks)

    return run
```

```python
import jax
import jax.numpy as jnp
from jax import lax
from jax.experimental import pallas as pl
from jax.experimental.pallas import tpu as pltpu
from jax.sharding import PartitionSpec as P

BINS = 1024
HALF = BINS // 2
LANES = 128
LOW = 32
WIRE = HALF + LANES

zfactor = 200.0
cos_zenith = 0.70710678
sin_zenith = 0.70710678
light_y = 0.70710678
HOT = jnp.float8_e4m3fn
STEPS = 65535.0


def bin_of(height):
    return jnp.clip(jnp.floor(height * 0.5), 0.0, BINS - 1.0)


def iota(shape, dim):
    return lax.broadcasted_iota(jnp.int32, shape, dim)


def in_vmem(x):
    return pltpu.with_memory_space_constraint(x, pltpu.VMEM)


def count_kernel(source, keep_ref, send_ref, heights, upper, lower, sems):
    rows, width = heights.shape
    part = width // sems.shape[0]
    copies = []
    for i in range(sems.shape[0]):
        some = slice(i * part, (i + 1) * part)
        copies.append(
            pltpu.make_async_copy(source.at[:, some], heights.at[:, some], sems.at[i])
        )
        copies[-1].start()
    for copy in copies:
        copy.wait()
    high_count = BINS // LOW
    bins = bin_of(heights[...])
    up = jnp.floor(bins * (1.0 / LOW))
    upper[...] = up
    lower[...] = bins - up * LOW
    row_ids = iota((LOW, width), 0).astype(jnp.float32).astype(jnp.bfloat16)
    one = jnp.array(1, HOT)
    zero = jnp.array(0, HOT)

    def hot(digits, r):
        again = digits[pl.ds(r, LOW // 2, stride=0), :].astype(jnp.bfloat16)
        return jnp.where(jnp.concatenate([again, again], axis=0) == row_ids, one, zero)

    grid = jnp.zeros((high_count, LOW), jnp.float32)
    for r in range(rows):
        grid = grid + lax.dot_general(
            hot(upper, r),
            hot(lower, r),
            (((1,), (1,)), ((), ())),
            preferred_element_type=jnp.float32,
        )
    tiled = jnp.concatenate([grid] * (LANES // LOW), axis=1)
    quarter = iota((high_count, LANES), 1) // LOW == iota((high_count, LANES), 0) % 4
    flat = jnp.where(quarter, tiled, 0.0)
    flat = flat + pltpu.roll(flat, high_count - 1, 0)
    flat = flat + pltpu.roll(flat, high_count - 2, 0)
    highest = jnp.max(heights[...])
    neg_lowest = -jnp.min(heights[...])
    first = lax.axis_index("row") & 1 == 0
    for i in range(4):
        cols = slice(i * LANES, (i + 1) * LANES)
        lower_row, upper_row = (flat[j : j + 1] for j in (4 * i, 4 * i + 16))
        keep_ref[:, cols] = jnp.where(first, lower_row, upper_row)
        send_ref[:, cols] = jnp.where(first, upper_row, lower_row)
    ends = jnp.where(iota((1, LANES), 1) < LANES // 2, highest, neg_lowest)
    keep_ref[:, HALF:] = ends
    send_ref[:, HALF:] = ends


VMEM_SPEC = pl.BlockSpec(memory_space=pltpu.VMEM)
SMALL = pltpu.CompilerParams(vmem_limit_bytes=16 * 2**20)


def count(elevation):
    shape = pltpu.VMEM((1, WIRE), jnp.float32)
    return pl.pallas_call(
        count_kernel,
        out_shape=(shape, shape, pltpu.VMEM(elevation.shape, jnp.float32)),
        in_specs=[pl.BlockSpec(memory_space=pltpu.HBM)],
        out_specs=(VMEM_SPEC,) * 3,
        scratch_shapes=[pltpu.VMEM(elevation.shape, jnp.float32)] * 2
        + [pltpu.SemaphoreType.DMA((4,))],
        name="count",
        compiler_params=SMALL,
    )(elevation)


def join_kernel(a_ref, b_ref, c_ref, d_ref, out_ref):
    a, b, c, d = a_ref[...], b_ref[...], c_ref[...], d_ref[...]
    added = (a + b) + (c + d)
    largest = jnp.maximum(jnp.maximum(a, b), jnp.maximum(c, d))
    joined = jnp.where(iota(a.shape, 1) < HALF, added, largest)
    out_ref[...] = jnp.broadcast_to(joined[None], out_ref.shape)


def join(a, b, c, d, copies):
    return pl.pallas_call(
        join_kernel,
        out_shape=pltpu.VMEM((copies, *a.shape), jnp.float32),
        in_specs=[VMEM_SPEC] * 4,
        out_specs=VMEM_SPEC,
        name="join",
        compiler_params=SMALL,
    )(a, b, c, d)


def gather_kernel(x_ref, out_ref):
    x = x_ref[...]
    out_ref[:, :HALF] = jnp.sum(x[:, :, :HALF], axis=0)
    out_ref[:, HALF:] = jnp.max(x[:, :, HALF:], axis=0)


def gather(everyone):
    return pl.pallas_call(
        gather_kernel,
        out_shape=pltpu.VMEM((1, WIRE), jnp.float32),
        in_specs=[VMEM_SPEC],
        out_specs=VMEM_SPEC,
        name="gather",
        compiler_params=SMALL,
    )(everyone)


def gradient_kernel(above, middle, below, ranks, gx_ref, gy_ref, bin_ref, rank_ref, wide):
    low, high = ranks[:, :1], ranks[:, 1:]
    rank_ref[:1] = jnp.broadcast_to(low, (1, LANES))
    rank_ref[1:] = jnp.broadcast_to(high - low, (1, LANES))
    rows, width = middle.shape
    halo = above.shape[0]
    edge = jnp.zeros((rows + 2 * halo, LANES), jnp.float32)
    wide[:, :LANES] = edge
    wide[:, LANES + width :] = edge
    wide[:halo, LANES : LANES + width] = above[...]
    wide[halo : halo + rows, LANES : LANES + width] = middle[...]
    wide[halo + rows :, LANES : LANES + width] = below[...]
    chunk = 4 * LANES
    tall = rows + 2 * halo
    for c in range(0, width, chunk):
        x = wide[:, LANES + c : LANES + c + chunk]
        for _ in range(7):
            x = x + pltpu.roll(x, tall - 1, 0)
        wide[:, LANES + c : LANES + c + chunk] = x * (1.0 / 4096)
    for c in range(0, width, chunk):
        x = wide[:, c : c + chunk + 2 * LANES]
        across = x.shape[1]

        def moved(k):
            return pltpu.roll(x, (-k) % across, 1)[:, LANES : LANES + chunk]

        right = [moved(k) for k in range(1, 5)]
        left = [moved(-k) for k in range(1, 5)]
        d1, d2, d3, d4 = (r - l for r, l in zip(right, left))
        s1, s2, s3, s4 = (r + l for r, l in zip(right, left))
        east = d4 + 6.0 * d3 + 14.0 * (d2 + d1)
        both = s4 + 8.0 * s3 + 28.0 * s2 + 56.0 * s1 + 70.0 * x[:, LANES : LANES + chunk]
        gx = east + pltpu.roll(east, tall - 1, 0)
        gy = pltpu.roll(both, tall - 1, 0) - both
        bin_ref[:, c : c + chunk] = bin_of(middle[:, c : c + chunk]).astype(jnp.int32)
        gx_ref[:, c : c + chunk] = gx[:rows]
        gy_ref[:, c : c + chunk] = gy[:rows]


def gradients(above, middle, below, ranks):
    rows, width = middle.shape
    shape = pltpu.VMEM(middle.shape, jnp.float32)
    return pl.pallas_call(
        gradient_kernel,
        out_shape=(
            shape,
            shape,
            pltpu.VMEM(middle.shape, jnp.int32),
            pltpu.VMEM((2, LANES), jnp.int32),
        ),
        in_specs=[VMEM_SPEC] * 4,
        out_specs=(VMEM_SPEC,) * 4,
        scratch_shapes=[
            pltpu.VMEM((rows + 2 * above.shape[0], width + 2 * LANES), jnp.float32)
        ],
        name="gradients",
        compiler_params=SMALL,
    )(above, middle, below, ranks)


def prefix_sums(counts):
    whole = counts.astype(jnp.int32)
    parts = [(whole >> shift) & 255 for shift in (0, 8, 16)]
    parts = jnp.concatenate(parts, axis=0).astype(jnp.float32).astype(jnp.bfloat16)
    upto = jnp.where(iota((LANES, LANES), 0) <= iota((LANES, LANES), 1), 1.0, 0.0)
    sums = jnp.dot(parts, upto.astype(jnp.bfloat16), preferred_element_type=jnp.float32)
    n = counts.shape[0]
    inside = sums[:n] + 256.0 * sums[n : 2 * n] + 65536.0 * sums[2 * n :]
    totals = jnp.broadcast_to(jnp.sum(counts, axis=1, keepdims=True), counts.shape)
    row_ids = iota(counts.shape, 0)
    for r in range(n - 1):
        inside = inside + jnp.where(row_ids > r, totals[r : r + 1], 0.0)
    return inside


def light_kernel(mine, gx_ref, gy_ref, out_ref):
    ends = mine[:, HALF:]
    span = ends + pltpu.roll(ends, LANES // 2, 1)
    scale = zfactor / (8.0 * span)
    for c in range(out_ref.shape[1] // LANES):
        cols = slice(c * LANES, (c + 1) * LANES)
        gx = gx_ref[:, cols] * scale
        gy = gy_ref[:, cols] * scale
        light = (cos_zenith - (sin_zenith * light_y) * (gy - gx)) * lax.rsqrt(
            1.0 + gx * gx + gy * gy
        )
        out_ref[:, cols] = 0.5 / STEPS + jnp.maximum(light, 0.0) * (1.0 / STEPS)


def lights(mine, gx, gy):
    return pl.pallas_call(
        light_kernel,
        out_shape=pltpu.VMEM(gx.shape, jnp.float32),
        in_specs=[VMEM_SPEC] * 3,
        out_specs=VMEM_SPEC,
        name="lights",
        compiler_params=SMALL,
    )(mine, gx, gy)


def shade_kernel(mine, theirs, limits, bins, lit, out_ref, done, sems):
    first = lax.axis_index("row") & 1 == 0
    a, b = mine[...], theirs[...]
    lower = jnp.where(first, a, b)
    upper = jnp.where(first, b, a)
    parts = [lower[:, i * LANES : (i + 1) * LANES] for i in range(4)]
    parts += [upper[:, i * LANES : (i + 1) * LANES] for i in range(4)]
    cumulative = prefix_sums(jnp.concatenate(parts, axis=0)).astype(jnp.int32)
    table = jnp.clip(
        (cumulative - limits[:1]).astype(jnp.float32) / limits[1:].astype(jnp.float32),
        0.0,
        1.0,
    )
    steps = jnp.floor(table * STEPS + 0.5).astype(jnp.int32)
    words = steps[:4] | (steps[4:] << 16)

    rows, width = bins.shape
    tables = [jnp.broadcast_to(words[r : r + 1], (rows, LANES)) for r in range(4)]
    pieces = sems.shape[0]
    piece = width // pieces
    copies = []
    for c in range(width // LANES):
        cols = slice(c * LANES, (c + 1) * LANES)
        code = bins[:, cols]
        low = code & (LANES - 1)
        w = [jnp.take_along_axis(t, low, axis=1, mode="promise_in_bounds") for t in tables]
        odd = (code & 128) != 0
        word = jnp.where((code & 256) != 0, jnp.where(odd, w[3], w[2]), jnp.where(odd, w[1], w[0]))
        stretch = ((word >> ((code >> 5) & 16)) & 65535).astype(jnp.float32)
        done[:, cols] = stretch * lit[:, cols]
        if (c + 1) * LANES % piece == 0:
            n = len(copies)
            span_cols = slice(n * piece, (n + 1) * piece)
            copies.append(
                pltpu.make_async_copy(done.at[:, span_cols], out_ref.at[:, span_cols], sems.at[n])
            )
            copies[-1].start()
    for copy in copies:
        copy.wait()


def shade(mine, theirs, limits, bins, lit):
    return pl.pallas_call(
        shade_kernel,
        out_shape=jax.ShapeDtypeStruct(lit.shape, jnp.float32),
        in_specs=[VMEM_SPEC] * 5,
        out_specs=pl.BlockSpec(memory_space=pl.ANY),
        scratch_shapes=[
            pltpu.VMEM(lit.shape, jnp.float32),
            pltpu.SemaphoreType.DMA((16,)),
        ],
        name="shade",
        compiler_params=SMALL,
    )(mine, theirs, limits, bins, lit)


def body(elevation, ranks):
    size = lax.axis_size("row")
    partner = [(i, i ^ 1) for i in range(size)]
    blocks = size // 4
    begin = blocks * 3 // 4
    order = [(i + begin) % blocks for i in range(blocks)]
    alike = [[4 * i + place for i in order] for place in range(4)]
    keep, send, local = count(pltpu.with_memory_space_constraint(elevation, pltpu.HBM))
    received = lax.ppermute(send, "row", partner)
    beside = lax.ppermute(keep, "row", [(i, i ^ 2) for i in range(size)])
    across = lax.ppermute(send, "row", [(i, i ^ 3) for i in range(size)])
    spread = join(
        in_vmem(keep), in_vmem(received), in_vmem(beside), in_vmem(across), blocks
    )
    everyone = lax.all_to_all(spread, "row", 0, 0, axis_index_groups=alike, tiled=True)

    above = lax.ppermute(local[-4:], "row", [(i, i + 1) for i in range(size - 1)])
    below = lax.ppermute(local[:4], "row", [(i + 1, i) for i in range(size - 1)])
    gx, gy, bins, limits = gradients(
        in_vmem(above), in_vmem(local), in_vmem(below), in_vmem(ranks.reshape(1, 2))
    )

    mine = gather(in_vmem(everyone))
    theirs = lax.ppermute(mine, "row", partner)
    lit = lights(in_vmem(mine), in_vmem(gx), in_vmem(gy))
    return shade(
        in_vmem(mine), in_vmem(theirs), in_vmem(limits), in_vmem(bins), in_vmem(lit)
    )


def solution(mesh):
    whole = P(("groups", "row"), None)
    mapped = jax.shard_map(
        body, mesh=mesh, in_specs=(whole, P("groups")), out_specs=whole, check_vma=False
    )

    def run(elevation, bin_index, ranks):
        return mapped(elevation, ranks)

    return run
```

```python
import jax
import jax.numpy as jnp
from jax import lax
from jax.experimental import pallas as pl
from jax.experimental.pallas import tpu as pltpu
from jax.sharding import PartitionSpec as P

BINS = 1024
HALF = BINS // 2
LANES = 128
LOW = 32
WIRE = HALF + LANES

zfactor = 200.0
cos_zenith = 0.70710678
sin_zenith = 0.70710678
light_y = 0.70710678
HOT = jnp.float8_e4m3fn
STEPS = 1023.0


def bin_of(height):
    return jnp.clip(jnp.floor(height * 0.5), 0.0, BINS - 1.0)


def iota(shape, dim):
    return lax.broadcasted_iota(jnp.int32, shape, dim)


def in_vmem(x):
    return pltpu.with_memory_space_constraint(x, pltpu.VMEM)


def count_kernel(source, keep_ref, send_ref, heights, upper, lower, sems):
    rows, width = heights.shape
    part = width // sems.shape[0]
    copies = []
    for i in range(sems.shape[0]):
        some = slice(i * part, (i + 1) * part)
        copies.append(
            pltpu.make_async_copy(source.at[:, some], heights.at[:, some], sems.at[i])
        )
        copies[-1].start()
    for copy in copies:
        copy.wait()
    high_count = BINS // LOW
    bins = bin_of(heights[...])
    up = jnp.floor(bins * (1.0 / LOW))
    upper[...] = up
    lower[...] = bins - up * LOW
    row_ids = iota((LOW, width), 0).astype(jnp.float32).astype(jnp.bfloat16)
    one = jnp.array(1, HOT)
    zero = jnp.array(0, HOT)

    def hot(digits, r):
        again = digits[pl.ds(r, LOW // 2, stride=0), :].astype(jnp.bfloat16)
        return jnp.where(jnp.concatenate([again, again], axis=0) == row_ids, one, zero)

    grid = jnp.zeros((high_count, LOW), jnp.float32)
    for r in range(rows):
        grid = grid + lax.dot_general(
            hot(upper, r),
            hot(lower, r),
            (((1,), (1,)), ((), ())),
            preferred_element_type=jnp.float32,
        )
    tiled = jnp.concatenate([grid] * (LANES // LOW), axis=1)
    quarter = iota((high_count, LANES), 1) // LOW == iota((high_count, LANES), 0) % 4
    flat = jnp.where(quarter, tiled, 0.0)
    flat = flat + pltpu.roll(flat, high_count - 1, 0)
    flat = flat + pltpu.roll(flat, high_count - 2, 0)
    highest = jnp.max(heights[...])
    neg_lowest = -jnp.min(heights[...])
    first = lax.axis_index("row") & 1 == 0
    for i in range(4):
        cols = slice(i * LANES, (i + 1) * LANES)
        lower_row, upper_row = (flat[j : j + 1] for j in (4 * i, 4 * i + 16))
        keep_ref[:, cols] = jnp.where(first, lower_row, upper_row)
        send_ref[:, cols] = jnp.where(first, upper_row, lower_row)
    ends = jnp.where(iota((1, LANES), 1) < LANES // 2, highest, neg_lowest)
    keep_ref[:, HALF:] = ends
    send_ref[:, HALF:] = ends


VMEM_SPEC = pl.BlockSpec(memory_space=pltpu.VMEM)
SMALL = pltpu.CompilerParams(vmem_limit_bytes=16 * 2**20)


def count(elevation):
    shape = pltpu.VMEM((1, WIRE), jnp.float32)
    return pl.pallas_call(
        count_kernel,
        out_shape=(shape, shape, pltpu.VMEM(elevation.shape, jnp.float32)),
        in_specs=[pl.BlockSpec(memory_space=pltpu.HBM)],
        out_specs=(VMEM_SPEC,) * 3,
        scratch_shapes=[pltpu.VMEM(elevation.shape, jnp.float32)] * 2
        + [pltpu.SemaphoreType.DMA((4,))],
        name="count",
        compiler_params=SMALL,
    )(elevation)


def join_kernel(a_ref, b_ref, c_ref, d_ref, out_ref):
    a, b, c, d = a_ref[...], b_ref[...], c_ref[...], d_ref[...]
    added = (a + b) + (c + d)
    largest = jnp.maximum(jnp.maximum(a, b), jnp.maximum(c, d))
    joined = jnp.where(iota(a.shape, 1) < HALF, added, largest)
    out_ref[...] = jnp.broadcast_to(joined[None], out_ref.shape)


def join(a, b, c, d, copies):
    return pl.pallas_call(
        join_kernel,
        out_shape=pltpu.VMEM((copies, *a.shape), jnp.float32),
        in_specs=[VMEM_SPEC] * 4,
        out_specs=VMEM_SPEC,
        name="join",
        compiler_params=SMALL,
    )(a, b, c, d)


def gather_kernel(x_ref, out_ref):
    x = x_ref[...]
    out_ref[:, :HALF] = jnp.sum(x[:, :, :HALF], axis=0)
    out_ref[:, HALF:] = jnp.max(x[:, :, HALF:], axis=0)


def gather(everyone):
    return pl.pallas_call(
        gather_kernel,
        out_shape=pltpu.VMEM((1, WIRE), jnp.float32),
        in_specs=[VMEM_SPEC],
        out_specs=VMEM_SPEC,
        name="gather",
        compiler_params=SMALL,
    )(everyone)


def gradient_kernel(above, middle, below, ranks, gx_ref, gy_ref, bin_ref, rank_ref, wide):
    low, high = ranks[:, :1], ranks[:, 1:]
    rank_ref[:1] = jnp.broadcast_to(low, (1, LANES))
    rank_ref[1:] = jnp.broadcast_to(high - low, (1, LANES))
    rows, width = middle.shape
    halo = above.shape[0]
    edge = jnp.zeros((rows + 2 * halo, LANES), jnp.float32)
    wide[:, :LANES] = edge
    wide[:, LANES + width :] = edge
    wide[:halo, LANES : LANES + width] = above[...]
    wide[halo : halo + rows, LANES : LANES + width] = middle[...]
    wide[halo + rows :, LANES : LANES + width] = below[...]
    chunk = 4 * LANES
    tall = rows + 2 * halo
    for c in range(0, width, chunk):
        x = wide[:, LANES + c : LANES + c + chunk]
        for _ in range(7):
            x = x + pltpu.roll(x, tall - 1, 0)
        wide[:, LANES + c : LANES + c + chunk] = x * (1.0 / 4096)
    for c in range(0, width, chunk):
        x = wide[:, c : c + chunk + 2 * LANES]
        across = x.shape[1]

        def moved(k):
            return pltpu.roll(x, (-k) % across, 1)[:, LANES : LANES + chunk]

        right = [moved(k) for k in range(1, 5)]
        left = [moved(-k) for k in range(1, 5)]
        d1, d2, d3, d4 = (r - l for r, l in zip(right, left))
        s1, s2, s3, s4 = (r + l for r, l in zip(right, left))
        east = d4 + 6.0 * d3 + 14.0 * (d2 + d1)
        both = s4 + 8.0 * s3 + 28.0 * s2 + 56.0 * s1 + 70.0 * x[:, LANES : LANES + chunk]
        gx = east + pltpu.roll(east, tall - 1, 0)
        gy = pltpu.roll(both, tall - 1, 0) - both
        bins = bin_of(middle[:, c : c + chunk]).astype(jnp.int32)
        row = bins >> 7
        word = jnp.where(row >= 6, 2, jnp.where(row >= 3, 1, 0))
        shift = (row - 3 * word) * 10
        bin_ref[:, c : c + chunk] = (bins & (LANES - 1)) | (word << 7) | (shift << 9)
        gx_ref[:, c : c + chunk] = gx[:rows]
        gy_ref[:, c : c + chunk] = gy[:rows]


def gradients(above, middle, below, ranks):
    rows, width = middle.shape
    shape = pltpu.VMEM(middle.shape, jnp.float32)
    return pl.pallas_call(
        gradient_kernel,
        out_shape=(
            shape,
            shape,
            pltpu.VMEM(middle.shape, jnp.int32),
            pltpu.VMEM((2, LANES), jnp.int32),
        ),
        in_specs=[VMEM_SPEC] * 4,
        out_specs=(VMEM_SPEC,) * 4,
        scratch_shapes=[
            pltpu.VMEM((rows + 2 * above.shape[0], width + 2 * LANES), jnp.float32)
        ],
        name="gradients",
        compiler_params=SMALL,
    )(above, middle, below, ranks)


def prefix_sums(counts):
    whole = counts.astype(jnp.int32)
    parts = [(whole >> shift) & 255 for shift in (0, 8, 16)]
    parts = jnp.concatenate(parts, axis=0).astype(jnp.float32).astype(jnp.bfloat16)
    upto = jnp.where(iota((LANES, LANES), 0) <= iota((LANES, LANES), 1), 1.0, 0.0)
    sums = jnp.dot(parts, upto.astype(jnp.bfloat16), preferred_element_type=jnp.float32)
    n = counts.shape[0]
    inside = sums[:n] + 256.0 * sums[n : 2 * n] + 65536.0 * sums[2 * n :]
    totals = jnp.broadcast_to(jnp.sum(counts, axis=1, keepdims=True), counts.shape)
    row_ids = iota(counts.shape, 0)
    for r in range(n - 1):
        inside = inside + jnp.where(row_ids > r, totals[r : r + 1], 0.0)
    return inside


def light_kernel(mine, gx_ref, gy_ref, out_ref):
    ends = mine[:, HALF:]
    span = ends + pltpu.roll(ends, LANES // 2, 1)
    scale = zfactor / (8.0 * span)
    for c in range(out_ref.shape[1] // LANES):
        cols = slice(c * LANES, (c + 1) * LANES)
        gx = gx_ref[:, cols] * scale
        gy = gy_ref[:, cols] * scale
        light = (cos_zenith - (sin_zenith * light_y) * (gy - gx)) * lax.rsqrt(
            1.0 + gx * gx + gy * gy
        )
        out_ref[:, cols] = 0.5 / STEPS + jnp.maximum(light, 0.0) * (1.0 / STEPS)


def lights(mine, gx, gy):
    return pl.pallas_call(
        light_kernel,
        out_shape=pltpu.VMEM(gx.shape, jnp.float32),
        in_specs=[VMEM_SPEC] * 3,
        out_specs=VMEM_SPEC,
        name="lights",
        compiler_params=SMALL,
    )(mine, gx, gy)


def shade_kernel(mine, theirs, limits, bins, lit, out_ref, done, sems):
    first = lax.axis_index("row") & 1 == 0
    a, b = mine[...], theirs[...]
    lower = jnp.where(first, a, b)
    upper = jnp.where(first, b, a)
    parts = [lower[:, i * LANES : (i + 1) * LANES] for i in range(4)]
    parts += [upper[:, i * LANES : (i + 1) * LANES] for i in range(4)]
    cumulative = prefix_sums(jnp.concatenate(parts, axis=0)).astype(jnp.int32)
    table = jnp.clip(
        (cumulative - limits[:1]).astype(jnp.float32) / limits[1:].astype(jnp.float32),
        0.0,
        1.0,
    )
    steps = jnp.floor(table * STEPS + 0.5).astype(jnp.int32)
    words = [
        steps[0:1] | (steps[1:2] << 10) | (steps[2:3] << 20),
        steps[3:4] | (steps[4:5] << 10) | (steps[5:6] << 20),
        steps[6:7] | (steps[7:8] << 10),
    ]

    rows, width = bins.shape
    tables = [jnp.broadcast_to(word, (rows, LANES)) for word in words]
    pieces = sems.shape[0]
    piece = width // pieces
    copies = []
    for c in range(width // LANES):
        cols = slice(c * LANES, (c + 1) * LANES)
        code = bins[:, cols]
        low = code & (LANES - 1)
        w = [jnp.take_along_axis(t, low, axis=1, mode="promise_in_bounds") for t in tables]
        word = jnp.where((code & 256) != 0, w[2], jnp.where((code & 128) != 0, w[1], w[0]))
        stretch = ((word >> (code >> 9)) & 1023).astype(jnp.float32)
        done[:, cols] = stretch * lit[:, cols]
        if (c + 1) * LANES % piece == 0:
            n = len(copies)
            span_cols = slice(n * piece, (n + 1) * piece)
            copies.append(
                pltpu.make_async_copy(done.at[:, span_cols], out_ref.at[:, span_cols], sems.at[n])
            )
            copies[-1].start()
    for copy in copies:
        copy.wait()


def shade(mine, theirs, limits, bins, lit):
    return pl.pallas_call(
        shade_kernel,
        out_shape=jax.ShapeDtypeStruct(lit.shape, jnp.float32),
        in_specs=[VMEM_SPEC] * 5,
        out_specs=pl.BlockSpec(memory_space=pl.ANY),
        scratch_shapes=[
            pltpu.VMEM(lit.shape, jnp.float32),
            pltpu.SemaphoreType.DMA((16,)),
        ],
        name="shade",
        compiler_params=SMALL,
    )(mine, theirs, limits, bins, lit)


def body(elevation, ranks):
    size = lax.axis_size("row")
    partner = [(i, i ^ 1) for i in range(size)]
    blocks = size // 4
    begin = blocks * 11 // 16
    order = [(i + begin) % blocks for i in range(blocks)]
    alike = [[4 * i + place for i in order] for place in range(4)]
    keep, send, local = count(pltpu.with_memory_space_constraint(elevation, pltpu.HBM))
    received = lax.ppermute(send, "row", partner)
    beside = lax.ppermute(keep, "row", [(i, i ^ 2) for i in range(size)])
    across = lax.ppermute(send, "row", [(i, i ^ 3) for i in range(size)])
    spread = join(
        in_vmem(keep), in_vmem(received), in_vmem(beside), in_vmem(across), blocks
    )
    everyone = lax.all_to_all(spread, "row", 0, 0, axis_index_groups=alike, tiled=True)

    above = lax.ppermute(local[-4:], "row", [(i, i + 1) for i in range(size - 1)])
    below = lax.ppermute(local[:4], "row", [(i + 1, i) for i in range(size - 1)])
    gx, gy, bins, limits = gradients(
        in_vmem(above), in_vmem(local), in_vmem(below), in_vmem(ranks.reshape(1, 2))
    )

    mine = gather(in_vmem(everyone))
    theirs = lax.ppermute(mine, "row", partner)
    lit = lights(in_vmem(mine), in_vmem(gx), in_vmem(gy))
    return shade(
        in_vmem(mine), in_vmem(theirs), in_vmem(limits), in_vmem(bins), in_vmem(lit)
    )


def solution(mesh):
    whole = P(("groups", "row"), None)
    mapped = jax.shard_map(
        body, mesh=mesh, in_specs=(whole, P("groups")), out_specs=whole, check_vma=False
    )

    def run(elevation, bin_index, ranks):
        return mapped(elevation, ranks)

    return run
```
